256 devices in a mesh: patch: 128 (over y, z, x), sub: 2 (over core).
Axes of the slice: x: 4, y: 4, z: 8, core: 2. Of those that a mesh axis runs over, the one named last changes fastest.
Arguments:
- fields: float32 [5, 512, 128, 128], P(None, ('patch', 'sub')), may hold values from -6 to 6
- density: float32 [512, 128, 128], P(('patch', 'sub')), may hold values from 1 to 3
- moduli: float32 [2, 512, 128, 128], P(None, ('patch', 'sub')), may hold values from 0.5 to 128
- metric_diag: float32 [2, 512, 128, 128], P(None, ('patch', 'sub')), may hold values from 0.7 to 1.3
- metric_cross: float32 [2, 512, 128, 128], P(None, ('patch', 'sub')), may hold values from -0.3 to 0.3
- fc_extension: float32 [25, 10], replicated, may hold values from -2 to 2
- patch_count: int32 [256], P(('patch', 'sub')), may hold values from 1 to 2, as said below
- connectivity: int32 [2048, 3], P(('patch', 'sub')), may hold values from -1 to 255, as said below
Outputs:
- advanced: float32 [5, 512, 128, 128], P(None, ('patch', 'sub'))
The draws below stay inside these ranges and needn't reach their ends.
Inputs may be any that keep to these rules, and one draw needn't show every extreme that they name: `patch_count`: every device holds at most 2 live patches; the largest count is 2 in every draw. `connectivity`: links join only live slots and are symmetric with equal orientation flags on both ends; a neighbour is held by the same device or by the device whose flat index differs by 1 or 129 modulo 256; from one device to another device go at most 2 linked sides, and this number is reached in every draw.
All inputs are finite; a program needn't handle non-finite values.
Results may differ from the reference program's by a relative error of at most 0.00005.
Values sent between devices are 32-bit elements; how exact they have to be, the bound alone decides.
No kernel may reach another device: no remote copies, remote signals or barrier semaphores. Data moves between devices by JAX's collectives and lax.ppermute only.
A program may use at most 64 MiB of HBM per device.

```python
import math
import jax
import jax.numpy as jnp
from jax import lax

N = 128
CONT = 25
MATCH = 5
PMAX = 2
STRIDE = 129
SLOTS = 512
DEVICES = 256


def patch_layout(key):
    base = jax.random.fold_in(key, 11)
    key_count, key_west, key_north = jax.random.split(base, 3)
    counts = jax.random.randint(key_count, (DEVICES,), max(1, PMAX // 4), PMAX + 1)
    counts = counts.at[0].set(PMAX).at[STRIDE].set(PMAX)
    west_flip = jax.random.randint(key_west, (DEVICES, PMAX), 0, 2)
    north_flip = jax.random.randint(key_north, (DEVICES, PMAX), 0, 2)
    return (counts.astype(jnp.int32), west_flip.astype(jnp.int32), north_flip.astype(jnp.int32))


def draw_patch_count(key, part):
    return patch_layout(key)[0]


def link_entry(linked, device_col, slot_col, side_value, flip_col):
    shape = (DEVICES, PMAX)
    linked = jnp.broadcast_to(linked, shape)
    device_col = jnp.broadcast_to(device_col, shape)
    slot_col = jnp.broadcast_to(slot_col, shape)
    flip_col = jnp.broadcast_to(flip_col, shape)
    return jnp.stack([jnp.where(linked, device_col, -1), jnp.where(linked, slot_col * 4 + side_value, 0), jnp.where(linked, flip_col, 0)], axis=-1)


def draw_connectivity(key, part):
    counts, west_flip, north_flip = patch_layout(key)
    device_ids = jnp.arange(DEVICES, dtype=jnp.int32)[:, None]
    slot_ids = jnp.arange(PMAX, dtype=jnp.int32)[None, :]
    held = counts[:, None]
    live = slot_ids < held
    before = (device_ids - 1) % DEVICES
    after = (device_ids + 1) % DEVICES
    above = (device_ids + STRIDE) % DEVICES
    below = (device_ids - STRIDE) % DEVICES
    first = slot_ids == 0
    last = slot_ids == held - 1
    west_dev = jnp.where(first, before, device_ids)
    west_slot = jnp.where(first, counts[before] - 1, slot_ids - 1)
    east_dev = jnp.where(last, after, device_ids)
    east_slot = jnp.where(last, 0, slot_ids + 1)
    next_index = jnp.broadcast_to(jnp.minimum(slot_ids + 1, PMAX - 1), (DEVICES, PMAX))
    inner_flip = jnp.take_along_axis(west_flip, next_index, axis=1)
    east_flip = jnp.where(last, west_flip[after[:, 0], 0][:, None], inner_flip)
    south_linked = live & (slot_ids < counts[below])
    north_linked = live & (slot_ids < counts[above])
    south_flip = north_flip[below[:, 0]]
    table = jnp.stack([link_entry(live, west_dev, west_slot, 1, west_flip), link_entry(live, east_dev, east_slot, 0, east_flip), link_entry(south_linked, below, slot_ids, 3, south_flip), link_entry(north_linked, above, slot_ids, 2, north_flip)], axis=2)
    return table.reshape(DEVICES * PMAX * 4, 3).astype(jnp.int32)


def draw_moduli(key, part):
    counts = patch_layout(key)[0]
    live_slots = (jnp.arange(PMAX, dtype=jnp.int32)[None, :] < counts[:, None]).reshape(SLOTS)
    key_patch, key_cell, key_dead = jax.random.split(jax.random.fold_in(key, 23), 3)
    top_factor = 4.0
    cell = jnp.exp(jax.random.uniform(key_cell, (2, SLOTS, N, N), jnp.float32, jnp.log(0.5), jnp.log(2.0)))
    live_factor = jnp.exp(jax.random.uniform(key_patch, (SLOTS,), jnp.float32) * jnp.log(top_factor))
    dead_factor = top_factor * jnp.exp(jax.random.uniform(key_dead, (SLOTS,), jnp.float32, jnp.log(2.0), jnp.log(4.0)))
    factor = jnp.where(live_slots, live_factor, dead_factor)
    return (factor[None, :, None, None] * cell).astype(jnp.float32)


def steps_of(rng, dims, pieces, smallest, largest):
    gain = 1.0
    for axis_at, blocks in pieces:
        draws = jax.random.uniform(jax.random.fold_in(jax.random.fold_in(rng, 6), axis_at), (blocks,), jnp.float32, smallest / len(pieces), largest / len(pieces))
        gain = gain * jnp.repeat(jnp.exp(draws), dims[axis_at] // blocks).reshape((-1,) + (1,) * (len(dims) - 1 - axis_at))
    return gain


def centred(key, dims, width, reach, cuts=(), held_as=jnp.bfloat16):
    factor_of = steps_of(key, dims, cuts, -0.22, 0.18) if cuts else 1.0
    entries = jax.random.normal(key, dims, jnp.float32) * width * factor_of
    return jnp.minimum(jnp.maximum(entries, -reach), reach).astype(held_as)


def setup_inputs(seed: int = 0) -> dict:
    keys = jax.random.split(jax.random.key(seed), 9)
    fields = centred(keys[0], (5, SLOTS, N, N), 1.0, 6.0, ((1, 256),), jnp.float32)
    density = jnp.clip(jnp.exp(math.log(3.0) - 1.0986123 * jax.random.uniform(keys[1], (SLOTS, N, N), jnp.float32) ** steps_of(keys[1], (SLOTS, N, N), ((0, 256),), -0.2, 0.2)), 1.0, 3.0)
    moduli = draw_moduli(jax.random.fold_in(keys[8], 71), 0)
    metric_diag = jnp.clip(0.7 + 0.59999996 * jax.random.uniform(keys[3], (2, SLOTS, N, N), jnp.float32) ** steps_of(keys[3], (2, SLOTS, N, N), ((1, 256),), -0.2, 0.2), 0.7, 1.3)
    metric_cross = jnp.clip(jax.random.uniform(keys[4], (2, SLOTS, N, N), jnp.float32, -0.3, 0.3) * steps_of(keys[4], (2, SLOTS, N, N), ((1, 256),), -0.4, 0.0), -0.3, 0.3)
    fc_extension = centred(keys[5], (CONT, 2 * MATCH), (2 * MATCH) ** -0.5, 2.0, (), jnp.float32)
    patch_count = draw_patch_count(jax.random.fold_in(keys[8], 71), 0)
    connectivity = draw_connectivity(jax.random.fold_in(keys[8], 71), 0)
    return dict(fields=fields, density=density, moduli=moduli, metric_diag=metric_diag, metric_cross=metric_cross, fc_extension=fc_extension, patch_count=patch_count, connectivity=connectivity)


cfl_number = 0.5
penalty_weight = 0.5

def wave_speed(density, moduli, metric_diag, metric_cross):
    stiff = moduli[0] + 2.0 * moduli[1]
    xi_norm = jnp.sqrt(metric_diag[0] * metric_diag[0] + metric_cross[0] * metric_cross[0])
    eta_norm = jnp.sqrt(metric_cross[1] * metric_cross[1] + metric_diag[1] * metric_diag[1])
    return jnp.sqrt(stiff / density) * (xi_norm + eta_norm)

def boundary_lines(state):
    stacked = jnp.stack([state[:, :, 0, :], state[:, :, -1, :], state[:, :, :, 0], state[:, :, :, -1]], axis=0)
    return jnp.transpose(stacked, (2, 0, 1, 3))

def assemble(state, along_xi, along_eta, partner_lines, side_mask, density, moduli, metric_diag, metric_cross):
    grad_x = metric_diag[0] * along_xi + metric_cross[1] * along_eta
    grad_y = metric_cross[0] * along_xi + metric_diag[1] * along_eta
    lame_first = moduli[0]
    shear = moduli[1]
    stiff = lame_first + 2.0 * shear
    rate_one = (grad_x[2] + grad_y[4]) / density
    rate_two = (grad_x[4] + grad_y[3]) / density
    rate_xx = stiff * grad_x[0] + lame_first * grad_y[1]
    rate_yy = lame_first * grad_x[0] + stiff * grad_y[1]
    rate_xy = shear * (grad_y[0] + grad_x[1])
    rate = jnp.stack([rate_one, rate_two, rate_xx, rate_yy, rate_xy], axis=0)
    points = state.shape[-1]
    jump = penalty_weight * (points - 1) * (partner_lines - boundary_lines(state)) * side_mask[:, :, None, None]
    jump = jnp.transpose(jump, (1, 2, 0, 3))
    rate = rate.at[:, :, 0, :].add(jump[0])
    rate = rate.at[:, :, points - 1, :].add(jump[1])
    rate = rate.at[:, :, :, 0].add(jump[2])
    rate = rate.at[:, :, :, points - 1].add(jump[3])
    return rate

def fc_derivative(values, extension, axis):
    moved = jnp.moveaxis(values, axis, -1)
    points = moved.shape[-1]
    match_pts = extension.shape[1] // 2
    tail = jnp.concatenate([moved[..., points - match_pts:], moved[..., :match_pts]], axis=-1)
    extra_vals = jnp.einsum('...m,cm->...c', tail, extension, precision=lax.Precision.HIGHEST)
    line = jnp.concatenate([moved, extra_vals], axis=-1)
    length = line.shape[-1]
    coeffs = jnp.fft.rfft(line, axis=-1)
    wave = 2.0 * jnp.pi * jnp.arange(length // 2 + 1, dtype=jnp.float32) * (points - 1) / length
    deriv = jnp.fft.irfft(coeffs * (1j * wave), n=length, axis=-1)[..., :points]
    return jnp.moveaxis(deriv.astype(values.dtype), -1, axis)

def reference(fields, density, moduli, metric_diag, metric_cross, fc_extension, patch_count, connectivity):
    state = fields.reshape(5, DEVICES, PMAX, N, N).transpose(1, 0, 2, 3, 4)
    dens_dev = density.reshape(DEVICES, PMAX, N, N)
    moduli_dev = moduli.reshape(2, DEVICES, PMAX, N, N).transpose(1, 0, 2, 3, 4)
    diag_dev = metric_diag.reshape(2, DEVICES, PMAX, N, N).transpose(1, 0, 2, 3, 4)
    cross_dev = metric_cross.reshape(2, DEVICES, PMAX, N, N).transpose(1, 0, 2, 3, 4)
    live = jnp.arange(PMAX, dtype=jnp.int32)[None, :] < patch_count[:, None]
    side_mask = (connectivity[:, 0] >= 0).astype(jnp.float32).reshape(DEVICES, PMAX, 4)

    def device_bound(device_data):
        speeds = wave_speed(device_data[0], device_data[1], device_data[2], device_data[3])
        return jnp.max(jnp.where(device_data[4][:, None, None], speeds, jnp.float32(0.0)))
    bound = jnp.max(lax.map(device_bound, (dens_dev, moduli_dev, diag_dev, cross_dev, live)))
    time_step = cfl_number / (bound * (N - 1))
    flat_target = (jnp.maximum(connectivity[:, 0], 0) * (PMAX * 4) + connectivity[:, 1]).astype(jnp.int32)
    flip_rows = connectivity[:, 2] == 1

    def partners(current):
        lines_all = jax.vmap(boundary_lines)(current).reshape(DEVICES * PMAX * 4, 5, N)
        picked = lines_all[flat_target]
        picked = jnp.where(flip_rows[:, None, None], picked[..., ::-1], picked)
        return picked.reshape(DEVICES, PMAX, 4, 5, N)

    def advance(current):
        near_lines = partners(current)

        def one_device(device_data):
            local = device_data[0]
            along_xi = fc_derivative(local, fc_extension, 2)
            along_eta = fc_derivative(local, fc_extension, 3)
            rate = assemble(local, along_xi, along_eta, device_data[1], device_data[2], device_data[3], device_data[4], device_data[5], device_data[6])
            return local + time_step * rate
        return lax.map(one_device, (current, near_lines, side_mask, dens_dev, moduli_dev, diag_dev, cross_dev))
    middle = advance(state)
    final = advance(middle)
    result = jnp.where(live[:, None, :, None, None], 0.5 * (state + final), jnp.float32(0.0))
    return result.transpose(1, 0, 2, 3, 4).reshape(5, SLOTS, N, N)
```

```python
import functools

import jax
import jax.numpy as jnp
import numpy as np
from jax import lax
from jax.experimental import pallas as pl
from jax.experimental.pallas import tpu as pltpu
from jax.sharding import Mesh
from jax.sharding import PartitionSpec as P

PATCH_SUB = ("patch_0", "patch_1", "patch_2", "sub")

CFL = 0.5
PENALTY = 0.5
CHUNK = 16
F32 = jnp.float32
BF16 = jnp.bfloat16
VMEM = pl.BlockSpec(memory_space=pltpu.VMEM)
SMEM = pl.BlockSpec(memory_space=pltpu.SMEM)
PARAMS = pltpu.CompilerParams(vmem_limit_bytes=12 * 1024 * 1024)


def fourier_matrix(points, cont):
    length = points + cont
    delta = np.arange(points)[:, None] - np.arange(length)[None, :]
    safe = np.where(delta == 0, 1, delta)
    scale = np.pi * (points - 1) / length
    sign = np.where(delta % 2 == 0, 1.0, -1.0)
    full = np.where(delta == 0, 0.0, scale * sign / np.sin(np.pi * safe / length))
    return full[:, :points].astype(np.float32), full[:, points:].astype(np.float32)


def pair_offsets(step):
    return (1, -1, step, -step)


def swap_routes(total, step):
    routes = []
    for offset in pair_offsets(step):
        route = []
        for i in range(total):
            target = (i + offset) % total if i % 2 == 0 else (i - offset) % total
            route.append((i, target))
        routes.append(route)
    return routes


def partner_ids(me, total, step):
    sign = jnp.where(me % 2 == 0, 1, -1)
    return [lax.rem(me + sign * offset + 2 * total, total) for offset in pair_offsets(step)]


def lane_ids(shape):
    return lax.broadcasted_iota(jnp.int32, shape, len(shape) - 1)


def extract_lines(load, own_ref, scr_ref, fields, slots, points):
    lanes = lane_ids((points, points))
    columns = jnp.zeros((points, points), F32)
    for s in range(slots):
        for f in range(fields):
            at = 2 * (s * fields + f)
            moved = pltpu.roll(load(f, s), at + 1, 1)
            columns = jnp.where((lanes == at) | (lanes == at + 1), moved, columns)
    scr_ref[...] = columns.T
    for s in range(slots):
        base = 2 * s * fields
        own_ref[4 * s + 2, pl.ds(0, fields), :] = scr_ref[pl.ds(base + 1, fields, stride=2), :]
        own_ref[4 * s + 3, pl.ds(0, fields), :] = scr_ref[pl.ds(base, fields, stride=2), :]


def fill_outboxes(own_ref, out_refs, conn_ref, partners):
    sides = own_ref.shape[0]
    for partner, out_ref in zip(partners, out_refs):
        first = jnp.int32(0)
        second = jnp.int32(0)
        count = jnp.int32(0)
        for i in range(sides):
            match = conn_ref[i, 0] == partner
            first = jnp.where(match & (count == 0), i, first)
            second = jnp.where(match & (count == 1), i, second)
            count = count + match.astype(jnp.int32)
        out_ref[0] = own_ref[first]
        out_ref[1] = own_ref[second]


def jumps(own_ref, in_refs, table_ref, jump_ref, conn_ref, me, partners, points, scale):
    sides = own_ref.shape[0]
    for i in range(sides):
        table_ref[i] = own_ref[i]
    for k, in_ref in enumerate(in_refs):
        table_ref[sides + 2 * k] = in_ref[0]
        table_ref[sides + 2 * k + 1] = in_ref[1]
    lanes = lane_ids((8, points))
    for i in range(sides):
        owner = conn_ref[i, 0]
        strip = conn_ref[i, 1]
        position = jnp.int32(0)
        for j in range(sides):
            if j != i:
                before = (conn_ref[j, 0] == owner) & (conn_ref[j, 1] < strip)
                position = position + before.astype(jnp.int32)
        place = strip
        for k, partner in enumerate(partners):
            place = jnp.where(owner == partner, sides + 2 * k + position, place)
        place = jnp.clip(place, 0, 2 * sides - 1)
        line = table_ref[place]
        index = jnp.where(conn_ref[i, 2] == 1, points - 1 - lanes, lanes)
        line = jnp.take_along_axis(line, index, axis=1)
        weight = jnp.where(owner >= 0, scale, 0.0).astype(F32)
        jump_ref[i] = weight * (line - own_ref[i])


def jump_columns(jump_ref, scr_ref, fields, slots, points):
    scr_ref[...] = jnp.zeros(scr_ref.shape, F32)
    for s in range(slots):
        base = 2 * s * fields
        for f in range(fields):
            scr_ref[pl.ds(base + 2 * f + 1, 1), :] = jump_ref[4 * s + 2, pl.ds(f, 1), :]
            scr_ref[pl.ds(base + 2 * f, 1), :] = jump_ref[4 * s + 3, pl.ds(f, 1), :]
    return scr_ref[...].T


def lines_kernel(
    fields_ref, density_ref, moduli_ref, diag_ref, cross_ref, conn_ref, count_ref, me_ref,
    out0, out1, out2, out3, own_ref, peak_ref, scr_ref, *, total, step,
):
    fields, slots, points, _ = fields_ref.shape
    for s in range(slots):
        for f in range(fields):
            own_ref[4 * s, pl.ds(f, 1), :] = fields_ref[f, s, pl.ds(0, 1), :]
            own_ref[4 * s + 1, pl.ds(f, 1), :] = fields_ref[f, s, pl.ds(points - 1, 1), :]
    extract_lines(lambda f, s: fields_ref[f, s], own_ref, scr_ref, fields, slots, points)
    fill_outboxes(own_ref, (out0, out1, out2, out3), conn_ref, partner_ids(me_ref[0], total, step))

    peak = jnp.zeros((8, points), F32)
    for s in range(slots):
        live = s < count_ref[0]

        def body(c, peak, s=s, live=live):
            rows = pl.ds(pl.multiple_of(c * CHUNK, CHUNK), CHUNK)
            stiff = moduli_ref[0, s, rows, :] + 2.0 * moduli_ref[1, s, rows, :]
            xi_x, eta_y = diag_ref[0, s, rows, :], diag_ref[1, s, rows, :]
            xi_y, eta_x = cross_ref[0, s, rows, :], cross_ref[1, s, rows, :]
            speed = jnp.sqrt(stiff / density_ref[s, rows, :]) * (
                jnp.sqrt(xi_x * xi_x + xi_y * xi_y) + jnp.sqrt(eta_x * eta_x + eta_y * eta_y)
            )
            speed = jnp.where(live, speed, 0.0)
            for r in range(CHUNK // 8):
                peak = jnp.maximum(peak, speed[8 * r : 8 * r + 8])
            return peak

        peak = lax.fori_loop(0, points // CHUNK, body, peak, unroll=True)
    row = jnp.max(peak, axis=0, keepdims=True)
    peak_ref[...] = jnp.broadcast_to(row, peak_ref.shape)


def matrix_kernel(inner_ref, outer_ref, ext_ref, left_ref, right_ref):
    points = inner_ref.shape[0]
    match = ext_ref.shape[1] // 2
    rows = lax.broadcasted_iota(jnp.int32, (2 * match, points), 0)
    lanes = lane_ids((2 * match, points))
    spread = jnp.where(lanes == jnp.where(rows < match, points - match + rows, rows - match), 1.0, 0.0)
    dot = functools.partial(
        jnp.dot, precision=lax.Precision.HIGHEST, preferred_element_type=F32
    )
    full = inner_ref[...] + dot(outer_ref[...], dot(ext_ref[...], spread.astype(F32)))
    high = full.astype(BF16)
    low = (full - high.astype(F32)).astype(BF16)
    zero = jnp.zeros((points, points), BF16)
    left_ref[pl.ds(0, points), pl.ds(0, points)] = high
    left_ref[pl.ds(0, points), pl.ds(points, points)] = high
    left_ref[pl.ds(points, points), pl.ds(0, points)] = low
    left_ref[pl.ds(points, points), pl.ds(points, points)] = zero
    turned = full.T
    high = turned.astype(BF16)
    low = (turned - high.astype(F32)).astype(BF16)
    right_ref[pl.ds(0, points), pl.ds(0, points)] = high
    right_ref[pl.ds(points, points), pl.ds(0, points)] = high
    right_ref[pl.ds(0, points), pl.ds(points, points)] = low
    right_ref[pl.ds(points, points), pl.ds(points, points)] = zero


def derivatives(load, left_ref, right_ref, cols_ref, rows_ref, xi_ref, eta_ref, fields, slots, points):
    for f in range(fields):
        for s in range(slots):
            value = load(f, s)
            high = value.astype(BF16)
            low = (value - high.astype(F32)).astype(BF16)
            cols_ref[f, pl.ds(0, points), pl.ds(s * points, points)] = high
            cols_ref[f, pl.ds(points, points), pl.ds(s * points, points)] = low
            rows_ref[f, pl.ds(s * points, points), pl.ds(0, points)] = high
            rows_ref[f, pl.ds(s * points, points), pl.ds(points, points)] = low
        got = jnp.dot(left_ref[...], cols_ref[f], preferred_element_type=F32)
        along = got[:points] + got[points:]
        for s in range(slots):
            xi_ref[f, s] = along[:, s * points : (s + 1) * points]
        got = jnp.dot(rows_ref[f], right_ref[...], preferred_element_type=F32)
        along = got[:, :points] + got[:, points:]
        for s in range(slots):
            eta_ref[f, s] = along[s * points : (s + 1) * points]


def assemble(s, rows, density_ref, moduli_ref, diag_ref, cross_ref, xi_ref, eta_ref):
    xi_x, eta_y = diag_ref[0, s, rows, :], diag_ref[1, s, rows, :]
    xi_y, eta_x = cross_ref[0, s, rows, :], cross_ref[1, s, rows, :]
    lame, shear = moduli_ref[0, s, rows, :], moduli_ref[1, s, rows, :]
    light = 1.0 / density_ref[s, rows, :]
    stiff = lame + 2.0 * shear

    def dx(f):
        return xi_x * xi_ref[f, s, rows, :] + eta_x * eta_ref[f, s, rows, :]

    def dy(f):
        return xi_y * xi_ref[f, s, rows, :] + eta_y * eta_ref[f, s, rows, :]

    one_x, two_y = dx(0), dy(1)
    return (
        (dx(2) + dy(4)) * light,
        (dx(4) + dy(3)) * light,
        stiff * one_x + lame * two_y,
        lame * one_x + stiff * two_y,
        shear * (dy(0) + dx(1)),
    )


def column_part(turned, at, points):
    moved = pltpu.roll(turned, points - 1 - at, 1)
    lanes = lane_ids(moved.shape)
    return jnp.where((lanes == 0) | (lanes == points - 1), moved, 0.0)


def first_kernel(
    fields_ref, density_ref, moduli_ref, diag_ref, cross_ref, left_ref, right_ref, own_ref,
    in0, in1, in2, in3, conn_ref, me_ref,
    rate_ref, out0, out1, out2, out3, mine_ref,
    table_ref, jump_ref, scr_ref, turned_ref, cols_ref, rows_ref, xi_ref, eta_ref, *, total, step, scale,
):
    fields, slots, points, _ = fields_ref.shape
    partners = partner_ids(me_ref[0], total, step)
    derivatives(
        lambda f, s: fields_ref[f, s], left_ref, right_ref, cols_ref, rows_ref, xi_ref, eta_ref, fields, slots, points
    )
    jumps(own_ref, (in0, in1, in2, in3), table_ref, jump_ref, conn_ref, me_ref[0], partners, points, scale)
    turned_ref[...] = jump_columns(jump_ref, scr_ref, fields, slots, points)
    for s in range(slots):
        for c in range(points // CHUNK):
            rows = pl.ds(c * CHUNK, CHUNK)
            parts = assemble(s, rows, density_ref, moduli_ref, diag_ref, cross_ref, xi_ref, eta_ref)
            for f in range(fields):
                rate_ref[f, s, rows, :] = parts[f] + column_part(turned_ref[rows, :], 2 * (s * fields + f), points)
        for f in range(fields):
            for side, row in ((0, 0), (1, points - 1)):
                line = rate_ref[f, s, pl.ds(row, 1), :] + jump_ref[4 * s + side, pl.ds(f, 1), :]
                rate_ref[f, s, pl.ds(row, 1), :] = line
                mine_ref[4 * s + side, pl.ds(f, 1), :] = line
    extract_lines(lambda f, s: rate_ref[f, s], mine_ref, scr_ref, fields, slots, points)
    fill_outboxes(mine_ref, (out0, out1, out2, out3), conn_ref, partners)


def second_kernel(
    fields_ref, rate_ref, density_ref, moduli_ref, diag_ref, cross_ref, left_ref, right_ref, peaks_ref, count_ref,
    new_ref, step_ref, cols_ref, rows_ref, xi_ref, eta_ref,
):
    fields, slots, points, _ = fields_ref.shape
    derivatives(
        lambda f, s: rate_ref[f, s], left_ref, right_ref, cols_ref, rows_ref, xi_ref, eta_ref, fields, slots, points
    )
    bound = jnp.max(peaks_ref[...], axis=0, keepdims=True)
    bound = jnp.max(bound, axis=1, keepdims=True)
    dt = CFL / (bound * (points - 1))
    half = 0.5 * dt * dt
    step_ref[...] = jnp.broadcast_to(half, step_ref.shape)
    for s in range(slots):
        live = s < count_ref[0]
        for c in range(points // CHUNK):
            rows = pl.ds(c * CHUNK, CHUNK)
            parts = assemble(s, rows, density_ref, moduli_ref, diag_ref, cross_ref, xi_ref, eta_ref)
            for f in range(fields):
                value = fields_ref[f, s, rows, :] + dt * rate_ref[f, s, rows, :] + half * parts[f]
                new_ref[f, s, rows, :] = jnp.where(live, value, 0.0)


def last_kernel(
    new_ref, half_ref, mine_ref, in0, in1, in2, in3, conn_ref, me_ref,
    final_ref, table_ref, jump_ref, scr_ref, turned_ref, *, total, step, scale,
):
    fields, slots, points, _ = new_ref.shape
    partners = partner_ids(me_ref[0], total, step)
    jumps(mine_ref, (in0, in1, in2, in3), table_ref, jump_ref, conn_ref, me_ref[0], partners, points, scale)
    for i in range(4 * slots):
        jump_ref[i] = jump_ref[i] * half_ref[...]
    turned_ref[...] = jump_columns(jump_ref, scr_ref, fields, slots, points)
    for s in range(slots):
        for f in range(fields):
            at = 2 * (s * fields + f)
            final_ref[f, s] = new_ref[f, s] + column_part(turned_ref[...], at, points)
            for side, row in ((0, 0), (1, points - 1)):
                line = final_ref[f, s, pl.ds(row, 1), :] + jump_ref[4 * s + side, pl.ds(f, 1), :]
                final_ref[f, s, pl.ds(row, 1), :] = line


def shards(fields, density, moduli, diag, cross, fc_extension, patch_count, connectivity):
    components, slots, points, _ = fields.shape
    total = lax.axis_size(PATCH_SUB)
    step = total // 2 + 1
    scale = PENALTY * (points - 1)
    sides = 4 * slots
    me = lax.axis_index(PATCH_SUB).reshape(1)
    inner, outer = fourier_matrix(points, fc_extension.shape[0])
    routes = swap_routes(total, step)

    box = jax.ShapeDtypeStruct((2, 8, points), F32)
    lines = jax.ShapeDtypeStruct((sides, 8, points), F32)
    grid = jax.ShapeDtypeStruct(fields.shape, F32)
    pair = jax.ShapeDtypeStruct((2 * points, 2 * points), BF16)
    square = pltpu.VMEM((points, points), F32)
    table = pltpu.VMEM((2 * sides, 8, points), F32)
    jump = pltpu.VMEM((sides, 8, points), F32)
    work = [
        pltpu.VMEM((components, 2 * points, 2 * points), BF16),
        pltpu.VMEM((components, 2 * points, 2 * points), BF16),
        pltpu.VMEM(fields.shape, F32),
        pltpu.VMEM(fields.shape, F32),
    ]

    def exchange(boxes):
        return [lax.ppermute(b, PATCH_SUB, r) for b, r in zip(boxes, routes)]

    *boxes, own, peak = pl.pallas_call(
        functools.partial(lines_kernel, total=total, step=step),
        out_shape=[box] * 4 + [lines, jax.ShapeDtypeStruct((total, points), F32)],
        in_specs=[VMEM] * 5 + [SMEM] * 3,
        out_specs=[VMEM] * 6,
        scratch_shapes=[square],
        compiler_params=PARAMS,
        name="lines",
    )(fields, density, moduli, diag, cross, connectivity, patch_count, me)
    arrived = exchange(boxes)
    peaks = lax.all_to_all(peak, PATCH_SUB, 0, 0, tiled=True)
    left, right = pl.pallas_call(
        matrix_kernel, out_shape=[pair, pair], in_specs=[VMEM] * 3, out_specs=[VMEM] * 2,
        compiler_params=PARAMS, name="matrix"
    )(jnp.asarray(inner), jnp.asarray(outer), fc_extension)
    rate, *boxes, mine = pl.pallas_call(
        functools.partial(first_kernel, total=total, step=step, scale=scale),
        out_shape=[grid] + [box] * 4 + [lines],
        in_specs=[VMEM] * 12 + [SMEM] * 2,
        out_specs=[VMEM] * 6,
        scratch_shapes=[table, jump, square, square] + work,
        compiler_params=PARAMS,
        name="first",
    )(fields, density, moduli, diag, cross, left, right, own, *arrived, connectivity, me)
    arrived = exchange(boxes)
    new, half = pl.pallas_call(
        second_kernel,
        out_shape=[grid, jax.ShapeDtypeStruct((8, points), F32)],
        in_specs=[VMEM] * 9 + [SMEM],
        out_specs=[VMEM] * 2,
        scratch_shapes=work,
        compiler_params=PARAMS,
        name="second",
    )(fields, rate, density, moduli, diag, cross, left, right, peaks, patch_count)
    return pl.pallas_call(
        functools.partial(last_kernel, total=total, step=step, scale=scale),
        out_shape=grid,
        in_specs=[VMEM] * 7 + [SMEM] * 2,
        out_specs=VMEM,
        scratch_shapes=[table, jump, square, square],
        compiler_params=PARAMS,
        name="last",
    )(new, half, mine, *arrived, connectivity, me)


def solution(mesh):
    torus = Mesh(
        mesh.devices.reshape(4, 8, 4, mesh.shape["sub"]), ("patch_0", "patch_1", "patch_2", "sub")
    )
    return jax.shard_map(
        shards,
        mesh=torus,
        in_specs=(
            P(None, PATCH_SUB, None, None),
            P(PATCH_SUB, None, None),
            P(None, PATCH_SUB, None, None),
            P(None, PATCH_SUB, None, None),
            P(None, PATCH_SUB, None, None),
            P(),
            P(PATCH_SUB),
            P(PATCH_SUB, None),
        ),
        out_specs=P(None, PATCH_SUB, None, None),
        check_vma=False,
    )
```

```python
import functools

import jax
import jax.numpy as jnp
import numpy as np
from jax import lax
from jax.experimental import pallas as pl
from jax.experimental.pallas import tpu as pltpu
from jax.sharding import Mesh
from jax.sharding import PartitionSpec as P

PATCH_SUB = ("patch_0", "patch_1", "patch_2", "sub")

CFL = 0.5
PENALTY = 0.5
CHUNK = 16
F32 = jnp.float32
BF16 = jnp.bfloat16
VMEM = pl.BlockSpec(memory_space=pltpu.VMEM)
SMEM = pl.BlockSpec(memory_space=pltpu.SMEM)
ANY = pl.BlockSpec(memory_space=pltpu.HBM)
PARAMS = pltpu.CompilerParams(vmem_limit_bytes=14 * 1024 * 1024)
CONN_LANE = 40
PEAK_LANE = 64


def fourier_matrix(points, cont):
    length = points + cont
    delta = np.arange(points)[:, None] - np.arange(length)[None, :]
    safe = np.where(delta == 0, 1, delta)
    scale = np.pi * (points - 1) / length
    sign = np.where(delta % 2 == 0, 1.0, -1.0)
    full = np.where(delta == 0, 0.0, scale * sign / np.sin(np.pi * safe / length))
    return full[:, :points].astype(np.float32), full[:, points:].astype(np.float32)


def offsets(total):
    step = total // 2 + 1
    return (1, -1, step, -step)


def lane_ids(shape):
    return lax.broadcasted_iota(jnp.int32, shape, len(shape) - 1)


def split(value):
    high = value.astype(BF16)
    return high, (value - high.astype(F32)).astype(BF16)


def boundary_columns(load, scr_ref, fields, slots, points):
    lanes = lane_ids((points, points))
    columns = jnp.zeros((points, points), F32)
    for s in range(slots):
        for f in range(fields):
            at = 2 * (s * fields + f)
            columns = jnp.where((lanes == at) | (lanes == at + 1), pltpu.roll(load(f, s), at + 1, 1), columns)
    scr_ref[...] = columns.T


def boundary_lines(ref, own_ref, row, scr_ref, fields, slots, points):
    boundary_columns(lambda f, s: ref[f, s], scr_ref, fields, slots, points)
    for s in range(slots):
        for f in range(fields):
            own_ref[4 * s, pl.ds(row + f, 1), :] = ref[f, s, pl.ds(0, 1), :]
            own_ref[4 * s + 1, pl.ds(row + f, 1), :] = ref[f, s, pl.ds(points - 1, 1), :]
        base = 2 * s * fields
        own_ref[4 * s + 2, pl.ds(row, fields), :] = scr_ref[pl.ds(base + 1, fields, stride=2), :]
        own_ref[4 * s + 3, pl.ds(row, fields), :] = scr_ref[pl.ds(base, fields, stride=2), :]


def column_part(turned, at, points):
    moved = pltpu.roll(turned, points - 1 - at, 1)
    lanes = lane_ids(moved.shape)
    return jnp.where((lanes == 0) | (lanes == points - 1), moved, 0.0)


def turn_jumps(jump_ref, scr_ref, fields, slots):
    for s in range(slots):
        for f in range(fields):
            at = 2 * (s * fields + f)
            scr_ref[pl.ds(at + 1, 1), :] = jump_ref[4 * s + 2, pl.ds(f, 1), :]
            scr_ref[pl.ds(at, 1), :] = jump_ref[4 * s + 3, pl.ds(f, 1), :]
    return scr_ref[...].T


def derivatives(f, value_of, left_ref, right_ref, cols_ref, rows_ref, xi_ref, eta_ref, slots, points):
    for s in range(slots):
        high, low = split(value_of(s))
        cols_ref[f, pl.ds(0, points), pl.ds(s * points, points)] = high
        cols_ref[f, pl.ds(points, points), pl.ds(s * points, points)] = low
        rows_ref[f, pl.ds(s * points, points), pl.ds(0, points)] = high
        rows_ref[f, pl.ds(s * points, points), pl.ds(points, points)] = low
    got = jnp.dot(left_ref[...], cols_ref[f], preferred_element_type=F32)
    along = got[:points] + got[points:]
    for s in range(slots):
        xi_ref[f, s] = along[:, s * points : (s + 1) * points]
    got = jnp.dot(rows_ref[f], right_ref[...], preferred_element_type=F32)
    along = got[:, :points] + got[:, points:]
    for s in range(slots):
        eta_ref[f, s] = along[s * points : (s + 1) * points]


def assemble(s, rows, density_ref, moduli_ref, diag_ref, cross_ref, xi_ref, eta_ref):
    xi_x, eta_y = diag_ref[0, s, rows, :], diag_ref[1, s, rows, :]
    xi_y, eta_x = cross_ref[0, s, rows, :], cross_ref[1, s, rows, :]
    lame, shear = moduli_ref[0, s, rows, :], moduli_ref[1, s, rows, :]
    light = 1.0 / density_ref[s, rows, :]
    stiff = lame + 2.0 * shear

    def dx(f):
        return xi_x * xi_ref[f, s, rows, :] + eta_x * eta_ref[f, s, rows, :]

    def dy(f):
        return xi_y * xi_ref[f, s, rows, :] + eta_y * eta_ref[f, s, rows, :]

    one_x, two_y = dx(0), dy(1)
    return (
        (dx(2) + dy(4)) * light,
        (dx(4) + dy(3)) * light,
        stiff * one_x + lame * two_y,
        lame * one_x + stiff * two_y,
        shear * (dy(0) + dx(1)),
    )


def build_matrices(inner, outer, ext, left_ref, right_ref):
    points = inner.shape[0]
    match = ext.shape[0] // 2
    rows = lax.broadcasted_iota(jnp.int32, (2 * match, points), 0)
    lanes = lane_ids((2 * match, points))
    place = jnp.where(rows < match, points - match + rows, rows - match)
    spread = jnp.where(lanes == place, 1.0, 0.0).astype(F32)
    exact = dict(precision=lax.Precision.HIGHEST, preferred_element_type=F32)
    wide = lax.dot_general(ext, spread, (((0,), (0,)), ((), ())), **exact)
    full = inner + jnp.dot(outer, wide, **exact)
    zero = jnp.zeros((points, points), BF16)
    first, second = pl.ds(0, points), pl.ds(points, points)
    high, low = split(full)
    left_ref[first, first] = high
    left_ref[first, second] = high
    left_ref[second, first] = low
    left_ref[second, second] = zero
    high, low = split(full.T)
    right_ref[first, first] = high
    right_ref[second, first] = high
    right_ref[first, second] = low
    right_ref[second, second] = zero


def front_kernel(
    fields_in, density_in, moduli_in, diag_in, cross_in, inner_in, outer_in, ext_in, conn_ref, count_ref, me_ref,
    out0, out1, out2, out3, own_ref, card_ref, rate_ref, left_ref, right_ref,
    fields_ref, density_ref, moduli_ref, diag_ref, cross_ref,
    inner_ref, outer_ref, ext_ref, scr_ref, cols_ref, rows_ref, xi_ref, eta_ref, sems, *, total,
):
    fields, slots, points, _ = fields_ref.shape
    sides = 4 * slots

    def fetch(source, target, at):
        copy = pltpu.make_async_copy(source, target, sems.at[at])
        copy.start()
        return copy

    small = [fetch(a, b, i) for i, (a, b) in enumerate(((inner_in, inner_ref), (outer_in, outer_ref), (ext_in, ext_ref)))]
    large = [fetch(fields_in.at[f], fields_ref.at[f], 3 + f) for f in range(fields)]
    coefs = [
        fetch(a, b, 3 + fields + i)
        for i, (a, b) in enumerate(
            ((density_in, density_ref), (moduli_in, moduli_ref), (diag_in, diag_ref), (cross_in, cross_ref))
        )
    ]
    for copy in small:
        copy.wait()
    build_matrices(inner_ref[...], outer_ref[...], ext_ref[...], left_ref, right_ref)
    for f in range(fields):
        large[f].wait()
        derivatives(
            f, lambda s, f=f: fields_ref[f, s], left_ref, right_ref, cols_ref, rows_ref, xi_ref, eta_ref, slots, points
        )
    boundary_lines(fields_ref, own_ref, 0, scr_ref, fields, slots, points)
    for copy in coefs:
        copy.wait()

    peak = jnp.zeros((8, points), F32)
    for s in range(slots):
        live = s < count_ref[0]
        for c in range(points // CHUNK):
            rows = pl.ds(c * CHUNK, CHUNK)
            stiff = moduli_ref[0, s, rows, :] + 2.0 * moduli_ref[1, s, rows, :]
            xi_x, eta_y = diag_ref[0, s, rows, :], diag_ref[1, s, rows, :]
            xi_y, eta_x = cross_ref[0, s, rows, :], cross_ref[1, s, rows, :]
            speed = jnp.sqrt(stiff / density_ref[s, rows, :]) * (
                jnp.sqrt(xi_x * xi_x + xi_y * xi_y) + jnp.sqrt(eta_x * eta_x + eta_y * eta_y)
            )
            speed = jnp.where(live, speed, 0.0)
            for r in range(CHUNK // 8):
                peak = jnp.maximum(peak, speed[8 * r : 8 * r + 8])
            parts = assemble(s, rows, density_ref, moduli_ref, diag_ref, cross_ref, xi_ref, eta_ref)
            for f in range(fields):
                rate_ref[f, s, rows, :] = parts[f]
    peak = jnp.max(jnp.max(peak, axis=0, keepdims=True), axis=1, keepdims=True)
    boundary_lines(rate_ref, own_ref, 8, scr_ref, fields, slots, points)

    lanes = lane_ids((8, points))
    corners = jnp.zeros((8, points), F32)
    for s in range(slots):
        for a in range(2):
            k = 4 * s + 2 * a
            moved = pltpu.roll(own_ref[4 * s + a, pl.ds(0, 8), :], k + 1, 1)
            corners = jnp.where((lanes == k) | (lanes == k + 1), moved, corners)
    scr_ref[pl.ds(0, 8), :] = corners
    lane = lane_ids((1, points))
    card = jnp.where(lane == PEAK_LANE, peak, 0.0)
    for f in range(fields):
        moved = pltpu.roll(scr_ref[pl.ds(f, 1), :], 8 * f, 1)
        card = jnp.where((lane >= 8 * f) & (lane < 8 * f + sides), moved, card)
    for i in range(sides):
        for c in range(3):
            card = jnp.where(lane == CONN_LANE + 3 * i + c, conn_ref[c, i].astype(F32), card)
    card_ref[...] = jnp.broadcast_to(card, card_ref.shape)

    for offset, out_ref in zip(offsets(total), (out0, out1, out2, out3)):
        partner = lax.rem(me_ref[0] + offset + total, total)
        first = jnp.int32(0)
        second = jnp.int32(0)
        count = jnp.int32(0)
        for i in range(sides):
            match = conn_ref[0, i] == partner
            first = jnp.where(match & (count == 0), i, first)
            second = jnp.where(match & (count == 1), i, second)
            count = count + match.astype(jnp.int32)
        out_ref[0] = own_ref[first]
        out_ref[1] = own_ref[second]


def corner_terms(cards_ref, conn_ref, near_ref, total, sides, points):
    shape = (2 * sides, points)
    rows = lax.broadcasted_iota(jnp.int32, shape, 0)
    lanes = lane_ids(shape)
    steps = (0,) + offsets(total)
    owner = jnp.zeros(shape, jnp.int32)
    strip = jnp.zeros(shape, jnp.int32)
    flip = jnp.zeros(shape, jnp.int32)
    for i in range(sides):
        here = rows // 2 == i
        held = jnp.maximum(conn_ref[0, i], 0)
        owner = jnp.where(here, held, owner)
        strip = jnp.where(here, conn_ref[1, i], strip)
        flip = jnp.where(here, conn_ref[2, i], flip)
        for d, offset in enumerate(steps):
            card = cards_ref[pl.ds(lax.rem(held + offset + total, total), 1), :]
            near_ref[d, pl.ds(2 * i, 1), :] = card
            near_ref[d, pl.ds(2 * i + 1, 1), :] = card

    def pick(array, index):
        return jnp.take_along_axis(array, index, axis=1)

    side = strip % 4
    base = strip - side
    at_end = jnp.where(rows % 2 == 0, 1 - flip, flip)
    across = side < 2
    other = jnp.where(across, 2 + at_end, at_end)
    odd = side % 2
    first = jnp.where(across, odd, at_end)
    second = jnp.where(across, at_end, odd)
    spread = 8 * jnp.minimum(lanes, 4)
    partner = near_ref[0]
    value = pick(partner, spread + base + 2 * first + 1 - second)
    link = CONN_LANE + 3 * (base + other)
    far_owner = pick(partner, link).astype(jnp.int32)
    far_strip = pick(partner, link + 1).astype(jnp.int32)
    far_flip = pick(partner, link + 2).astype(jnp.int32)
    far_card = partner
    for d, offset in enumerate(steps):
        if d:
            far_card = jnp.where(far_owner == lax.rem(owner + offset + total, total), near_ref[d], far_card)
    far_side = far_strip % 4
    far_base = far_strip - far_side
    point = jnp.where(far_flip == 1, 1 - odd, odd)
    far_across = far_side < 2
    far_odd = far_side % 2
    far_first = jnp.where(far_across, far_odd, point)
    far_second = jnp.where(far_across, point, far_odd)
    beyond = pick(far_card, spread + far_base + 2 * far_first + 1 - far_second)
    return jnp.where(far_owner >= 0, beyond - value, 0.0)


def last_kernel(
    fields_ref, inside_ref, density_ref, moduli_ref, diag_ref, cross_ref, left_ref, right_ref, own_ref, cards_ref,
    in0, in1, in2, in3, conn_ref, count_ref, me_ref,
    final_out,
    table_ref, jump_ref, mine_ref, near_ref, scr_ref, turned_ref, corner_ref,
    cols_ref, rows_ref, xi_ref, eta_ref, rate_ref, final_ref, sems, *, total, scale,
):
    fields, slots, points, _ = fields_ref.shape
    sides = 4 * slots
    lanes = lane_ids((8, points))
    scr_ref[...] = jnp.zeros(scr_ref.shape, F32)

    for i in range(sides):
        table_ref[i] = own_ref[i]
    for k, in_ref in enumerate((in0, in1, in2, in3)):
        table_ref[sides + 2 * k] = in_ref[0]
        table_ref[sides + 2 * k + 1] = in_ref[1]
    weights = []
    partner_rates = []
    for i in range(sides):
        owner = conn_ref[0, i]
        strip = conn_ref[1, i]
        position = jnp.int32(0)
        for j in range(sides):
            if j != i:
                before = (conn_ref[0, j] == owner) & (conn_ref[1, j] < strip)
                position = position + before.astype(jnp.int32)
        place = strip
        for k, offset in enumerate(offsets(total)):
            source = lax.rem(me_ref[0] - offset + total, total)
            place = jnp.where(owner == source, sides + 2 * k + position, place)
        place = jnp.clip(place, 0, 2 * sides - 1)
        index = jnp.where(conn_ref[2, i] == 1, points - 1 - lanes, lanes)
        line = jnp.take_along_axis(table_ref[place, pl.ds(0, 8), :], index, axis=1)
        rate = jnp.take_along_axis(table_ref[place, pl.ds(8, 8), :], index, axis=1)
        weight = jnp.where(owner >= 0, scale, 0.0).astype(F32)
        jump = weight * (line - own_ref[i, pl.ds(0, 8), :])
        jump_ref[i] = jump
        weights.append(weight)
        partner_rates.append(rate - jump)
    turned_ref[...] = turn_jumps(jump_ref, scr_ref, fields, slots)

    for f in range(fields):
        for s in range(slots):
            rate_ref[f, s] = inside_ref[f, s] + column_part(turned_ref[...], 2 * (s * fields + f), points)
            for side, row in ((0, 0), (1, points - 1)):
                line = rate_ref[f, s, pl.ds(row, 1), :] + jump_ref[4 * s + side, pl.ds(f, 1), :]
                rate_ref[f, s, pl.ds(row, 1), :] = line
        derivatives(
            f, lambda s, f=f: rate_ref[f, s], left_ref, right_ref, cols_ref, rows_ref, xi_ref, eta_ref, slots, points
        )
    boundary_lines(rate_ref, mine_ref, 0, scr_ref, fields, slots, points)

    bound = jnp.max(cards_ref[...], axis=0, keepdims=True)
    bound = jnp.where(lane_ids(bound.shape) == PEAK_LANE, bound, 0.0)
    bound = jnp.max(bound, axis=1, keepdims=True)
    dt = CFL / (bound * (points - 1))
    half = 0.5 * dt * dt

    corner_ref[...] = jnp.zeros(corner_ref.shape, F32)
    corner_ref[pl.ds(0, 2 * sides), :] = corner_terms(cards_ref, conn_ref, near_ref, total, sides, points)
    corners = corner_ref[...].T[:8]
    for i in range(sides):
        partner = partner_rates[i] + scale * column_part(corners, 2 * i, points)
        jump_ref[i] = half * weights[i] * (partner - mine_ref[i])
    turned_ref[...] = turn_jumps(jump_ref, scr_ref, fields, slots)

    copies = []
    for s in range(slots):
        live = s < count_ref[0]
        for c in range(points // CHUNK):
            rows = pl.ds(c * CHUNK, CHUNK)
            parts = assemble(s, rows, density_ref, moduli_ref, diag_ref, cross_ref, xi_ref, eta_ref)
            for f in range(fields):
                value = fields_ref[f, s, rows, :] + dt * rate_ref[f, s, rows, :] + half * parts[f]
                value = value + column_part(turned_ref[rows, :], 2 * (s * fields + f), points)
                final_ref[f, s, rows, :] = jnp.where(live, value, 0.0)
        for f in range(fields):
            for side, row in ((0, 0), (1, points - 1)):
                line = final_ref[f, s, pl.ds(row, 1), :] + jump_ref[4 * s + side, pl.ds(f, 1), :]
                final_ref[f, s, pl.ds(row, 1), :] = jnp.where(live, line, 0.0)
            copy = pltpu.make_async_copy(final_ref.at[f, s], final_out.at[f, s], sems.at[s * fields + f])
            copy.start()
            copies.append(copy)
    for copy in copies:
        copy.wait()


def shards(fields, density, moduli, diag, cross, fc_extension, patch_count, connectivity):
    components, slots, points, _ = fields.shape
    total = lax.axis_size(PATCH_SUB)
    scale = PENALTY * (points - 1)
    sides = 4 * slots
    me = lax.axis_index(PATCH_SUB).reshape(1)
    cont = fc_extension.shape[0]
    inner, outer = fourier_matrix(points, cont)
    links = connectivity.T

    def stay(x):
        return pltpu.with_memory_space_constraint(jnp.asarray(x), pltpu.HBM)

    def like(x):
        return jax.ShapeDtypeStruct(x.shape, x.dtype)

    box = jax.ShapeDtypeStruct((2, 16, points), F32)
    pair = jax.ShapeDtypeStruct((2 * points, 2 * points), BF16)
    square = pltpu.VMEM((points, points), F32)
    parts = pltpu.VMEM((components, 2 * points, 2 * points), BF16)
    grid = pltpu.VMEM(fields.shape, F32)

    (b0, b1, b2, b3, own, card, rate, left, right, fields, density, moduli, diag, cross) = pl.pallas_call(
        functools.partial(front_kernel, total=total),
        out_shape=[box] * 4
        + [
            jax.ShapeDtypeStruct((sides, 16, points), F32),
            jax.ShapeDtypeStruct((total, points), F32),
            like(fields),
            pair,
            pair,
        ]
        + [like(x) for x in (fields, density, moduli, diag, cross)],
        in_specs=[ANY] * 8 + [SMEM] * 3,
        out_specs=[VMEM] * 14,
        scratch_shapes=[
            square,
            pltpu.VMEM((points, cont), F32),
            pltpu.VMEM((fc_extension.shape[1], cont), F32),
            square,
            parts,
            parts,
            grid,
            grid,
            pltpu.SemaphoreType.DMA((7 + components,)),
        ],
        compiler_params=PARAMS,
        name="front",
    )(*[stay(x) for x in (fields, density, moduli, diag, cross, inner, outer, fc_extension.T)], links, patch_count, me)
    cards = lax.all_to_all(card, PATCH_SUB, 0, 0, tiled=True)
    arrived = [
        lax.ppermute(b, PATCH_SUB, [(i, (i + offset) % total) for i in range(total)])
        for b, offset in zip((b0, b1, b2, b3), offsets(total))
    ]
    line = pltpu.VMEM((sides, 8, points), F32)
    return pl.pallas_call(
        functools.partial(last_kernel, total=total, scale=scale),
        out_shape=like(fields),
        in_specs=[VMEM] * 14 + [SMEM] * 3,
        out_specs=ANY,
        scratch_shapes=[
            pltpu.VMEM((2 * sides, 16, points), F32),
            line,
            line,
            pltpu.VMEM((5, 2 * sides, points), F32),
            square,
            square,
            square,
            parts,
            parts,
            grid,
            grid,
            grid,
            grid,
            pltpu.SemaphoreType.DMA((components * slots,)),
        ],
        compiler_params=PARAMS,
        name="last",
    )(fields, rate, density, moduli, diag, cross, left, right, own, cards, *arrived, links, patch_count, me)


def solution(mesh):
    torus = Mesh(
        mesh.devices.reshape(4, 8, 4, mesh.shape["sub"]), ("patch_0", "patch_1", "patch_2", "sub")
    )
    return jax.shard_map(
        shards,
        mesh=torus,
        in_specs=(
            P(None, PATCH_SUB, None, None),
            P(PATCH_SUB, None, None),
            P(None, PATCH_SUB, None, None),
            P(None, PATCH_SUB, None, None),
            P(None, PATCH_SUB, None, None),
            P(),
            P(PATCH_SUB),
            P(PATCH_SUB, None),
        ),
        out_specs=P(None, PATCH_SUB, None, None),
        check_vma=False,
    )
```

```python
import functools

import jax
import jax.numpy as jnp
import numpy as np
from jax import lax
from jax.experimental import pallas as pl
from jax.experimental.pallas import tpu as pltpu
from jax.sharding import Mesh
from jax.sharding import PartitionSpec as P

PATCH_SUB = ("patch_0", "patch_1", "patch_2", "sub")

CFL = 0.5
PENALTY = 0.5
CHUNK = 16
F32 = jnp.float32
BF16 = jnp.bfloat16
VMEM = pl.BlockSpec(memory_space=pltpu.VMEM)
SMEM = pl.BlockSpec(memory_space=pltpu.SMEM)
ANY = pl.BlockSpec(memory_space=pltpu.HBM)
PARAMS = pltpu.CompilerParams(vmem_limit_bytes=14 * 1024 * 1024)
CONN_LANE = 40
PEAK_LANE = 64


def fourier_matrix(points, cont):
    length = points + cont
    delta = np.arange(points)[:, None] - np.arange(length)[None, :]
    safe = np.where(delta == 0, 1, delta)
    scale = np.pi * (points - 1) / length
    sign = np.where(delta % 2 == 0, 1.0, -1.0)
    full = np.where(delta == 0, 0.0, scale * sign / np.sin(np.pi * safe / length))
    return full[:, :points].astype(np.float32), full[:, points:].astype(np.float32)


def offsets(total):
    step = total // 2 + 1
    return (1, -1, step, -step)


ORDER = (3, 1, 2, 0)


def routes(total):
    return [
        [(i, (i + (offset if i % 2 == 0 else -offset)) % total) for i in range(total)]
        for offset in (offsets(total)[k] for k in ORDER)
    ]


def partners(me, total):
    sign = jnp.where(lax.rem(me, 2) == 0, 1, -1)
    return [lax.rem(me + sign * offsets(total)[k] + total, total) for k in ORDER]


def lane_ids(shape):
    return lax.broadcasted_iota(jnp.int32, shape, len(shape) - 1)


def split(value):
    high = value.astype(BF16)
    return high, (value - high.astype(F32)).astype(BF16)


def boundary_columns(load, scr_ref, fields, slots, points):
    lanes = lane_ids((points, points))
    columns = jnp.zeros((points, points), F32)
    for s in range(slots):
        for f in range(fields):
            at = 2 * (s * fields + f)
            columns = jnp.where((lanes == at) | (lanes == at + 1), pltpu.roll(load(f, s), at + 1, 1), columns)
    scr_ref[...] = columns.T


def boundary_lines(ref, own_ref, row, scr_ref, fields, slots, points):
    boundary_columns(lambda f, s: ref[f, s], scr_ref, fields, slots, points)
    for s in range(slots):
        for f in range(fields):
            own_ref[4 * s, pl.ds(row + f, 1), :] = ref[f, s, pl.ds(0, 1), :]
            own_ref[4 * s + 1, pl.ds(row + f, 1), :] = ref[f, s, pl.ds(points - 1, 1), :]
        base = 2 * s * fields
        own_ref[4 * s + 2, pl.ds(row, fields), :] = scr_ref[pl.ds(base + 1, fields, stride=2), :]
        own_ref[4 * s + 3, pl.ds(row, fields), :] = scr_ref[pl.ds(base, fields, stride=2), :]


def column_part(turned, at, points):
    moved = pltpu.roll(turned, points - 1 - at, 1)
    lanes = lane_ids(moved.shape)
    return jnp.where((lanes == 0) | (lanes == points - 1), moved, 0.0)


def turn_jumps(jump_ref, scr_ref, fields, slots):
    for s in range(slots):
        for f in range(fields):
            at = 2 * (s * fields + f)
            scr_ref[pl.ds(at + 1, 1), :] = jump_ref[4 * s + 2, pl.ds(f, 1), :]
            scr_ref[pl.ds(at, 1), :] = jump_ref[4 * s + 3, pl.ds(f, 1), :]
    return scr_ref[...].T


def derivatives(f, value_of, left_ref, right_ref, cols_ref, rows_ref, xi_ref, eta_ref, slots, points):
    for s in range(slots):
        high, low = split(value_of(s))
        cols_ref[f, pl.ds(0, points), pl.ds(s * points, points)] = high
        cols_ref[f, pl.ds(points, points), pl.ds(s * points, points)] = low
        rows_ref[f, pl.ds(s * points, points), pl.ds(0, points)] = high
        rows_ref[f, pl.ds(s * points, points), pl.ds(points, points)] = low
    got = jnp.dot(left_ref[...], cols_ref[f], preferred_element_type=F32)
    along = got[:points] + got[points:]
    for s in range(slots):
        xi_ref[f, s] = along[:, s * points : (s + 1) * points]
    got = jnp.dot(rows_ref[f], right_ref[...], preferred_element_type=F32)
    along = got[:, :points] + got[:, points:]
    for s in range(slots):
        eta_ref[f, s] = along[s * points : (s + 1) * points]


def assemble(s, rows, density_ref, moduli_ref, diag_ref, cross_ref, xi_ref, eta_ref):
    xi_x, eta_y = diag_ref[0, s, rows, :], diag_ref[1, s, rows, :]
    xi_y, eta_x = cross_ref[0, s, rows, :], cross_ref[1, s, rows, :]
    lame, shear = moduli_ref[0, s, rows, :], moduli_ref[1, s, rows, :]
    light = 1.0 / density_ref[s, rows, :]
    stiff = lame + 2.0 * shear

    def dx(f):
        return xi_x * xi_ref[f, s, rows, :] + eta_x * eta_ref[f, s, rows, :]

    def dy(f):
        return xi_y * xi_ref[f, s, rows, :] + eta_y * eta_ref[f, s, rows, :]

    one_x, two_y = dx(0), dy(1)
    return (
        (dx(2) + dy(4)) * light,
        (dx(4) + dy(3)) * light,
        stiff * one_x + lame * two_y,
        lame * one_x + stiff * two_y,
        shear * (dy(0) + dx(1)),
    )


def build_matrices(inner, outer, ext, left_ref, right_ref):
    points = inner.shape[0]
    match = ext.shape[0] // 2
    rows = lax.broadcasted_iota(jnp.int32, (2 * match, points), 0)
    lanes = lane_ids((2 * match, points))
    place = jnp.where(rows < match, points - match + rows, rows - match)
    spread = jnp.where(lanes == place, 1.0, 0.0).astype(F32)
    exact = dict(precision=lax.Precision.HIGHEST, preferred_element_type=F32)
    wide = lax.dot_general(ext, spread, (((0,), (0,)), ((), ())), **exact)
    full = inner + jnp.dot(outer, wide, **exact)
    zero = jnp.zeros((points, points), BF16)
    first, second = pl.ds(0, points), pl.ds(points, points)
    high, low = split(full)
    left_ref[first, first] = high
    left_ref[first, second] = high
    left_ref[second, first] = low
    left_ref[second, second] = zero
    high, low = split(full.T)
    right_ref[first, first] = high
    right_ref[second, first] = high
    right_ref[first, second] = low
    right_ref[second, second] = zero


def front_kernel(
    fields_in, density_in, moduli_in, diag_in, cross_in, inner_in, outer_in, ext_in, conn_in, count_ref,
    out0, out1, out2, out3, own_ref, card_ref, rate_ref, left_ref, right_ref,
    fields_ref, density_ref, moduli_ref, diag_ref, cross_ref, links_ref,
    inner_ref, outer_ref, ext_ref, scr_ref, cols_ref, rows_ref, xi_ref, eta_ref, conn_ref, sems, *, total,
):
    fields, slots, points, _ = fields_ref.shape
    sides = 4 * slots

    def fetch(source, target, at):
        copy = pltpu.make_async_copy(source, target, sems.at[at])
        copy.start()
        return copy

    small = [fetch(a, b, i) for i, (a, b) in enumerate(((inner_in, inner_ref), (outer_in, outer_ref), (ext_in, ext_ref)))]
    large = [fetch(fields_in.at[f], fields_ref.at[f], 3 + f) for f in range(fields)]
    coefs = [
        fetch(a, b, 3 + fields + i)
        for i, (a, b) in enumerate(
            ((density_in, density_ref), (moduli_in, moduli_ref), (diag_in, diag_ref), (cross_in, cross_ref))
        )
    ]
    links = [fetch(conn_in, conn_ref, 7 + fields), fetch(conn_in, links_ref, 8 + fields)]
    for copy in small:
        copy.wait()
    build_matrices(inner_ref[...], outer_ref[...], ext_ref[...], left_ref, right_ref)
    for f in range(fields):
        large[f].wait()
        derivatives(
            f, lambda s, f=f: fields_ref[f, s], left_ref, right_ref, cols_ref, rows_ref, xi_ref, eta_ref, slots, points
        )
    boundary_lines(fields_ref, own_ref, 0, scr_ref, fields, slots, points)
    for copy in coefs + links:
        copy.wait()

    peak = jnp.zeros((8, points), F32)
    for s in range(slots):
        live = s < count_ref[0]
        for c in range(points // CHUNK):
            rows = pl.ds(c * CHUNK, CHUNK)
            stiff = moduli_ref[0, s, rows, :] + 2.0 * moduli_ref[1, s, rows, :]
            xi_x, eta_y = diag_ref[0, s, rows, :], diag_ref[1, s, rows, :]
            xi_y, eta_x = cross_ref[0, s, rows, :], cross_ref[1, s, rows, :]
            speed = jnp.sqrt(stiff / density_ref[s, rows, :]) * (
                jnp.sqrt(xi_x * xi_x + xi_y * xi_y) + jnp.sqrt(eta_x * eta_x + eta_y * eta_y)
            )
            speed = jnp.where(live, speed, 0.0)
            for r in range(CHUNK // 8):
                peak = jnp.maximum(peak, speed[8 * r : 8 * r + 8])
            parts = assemble(s, rows, density_ref, moduli_ref, diag_ref, cross_ref, xi_ref, eta_ref)
            for f in range(fields):
                rate_ref[f, s, rows, :] = parts[f]
    peak = jnp.max(jnp.max(peak, axis=0, keepdims=True), axis=1, keepdims=True)
    boundary_lines(rate_ref, own_ref, 8, scr_ref, fields, slots, points)

    lanes = lane_ids((8, points))
    corners = jnp.zeros((8, points), F32)
    for s in range(slots):
        for a in range(2):
            k = 4 * s + 2 * a
            moved = pltpu.roll(own_ref[4 * s + a, pl.ds(0, 8), :], k + 1, 1)
            corners = jnp.where((lanes == k) | (lanes == k + 1), moved, corners)
    scr_ref[pl.ds(0, 8), :] = corners
    lane = lane_ids((1, points))
    card = jnp.where(lane == PEAK_LANE, peak, 0.0)
    for f in range(fields):
        moved = pltpu.roll(scr_ref[pl.ds(f, 1), :], 8 * f, 1)
        card = jnp.where((lane >= 8 * f) & (lane < 8 * f + sides), moved, card)
    for i in range(sides):
        for c in range(3):
            card = jnp.where(lane == CONN_LANE + 3 * i + c, conn_ref[c, i].astype(F32), card)
    card_ref[...] = jnp.broadcast_to(card, card_ref.shape)

    for partner, out_ref in zip(partners(lax.axis_index(PATCH_SUB), total), (out0, out1, out2, out3)):
        first = jnp.int32(0)
        second = jnp.int32(0)
        count = jnp.int32(0)
        for i in range(sides):
            match = conn_ref[0, i] == partner
            first = jnp.where(match & (count == 0), i, first)
            second = jnp.where(match & (count == 1), i, second)
            count = count + match.astype(jnp.int32)
        out_ref[0] = own_ref[first]
        out_ref[1] = own_ref[second]


def corner_terms(cards_ref, conn_ref, near_ref, total, sides, points):
    shape = (2 * sides, points)
    rows = lax.broadcasted_iota(jnp.int32, shape, 0)
    lanes = lane_ids(shape)
    steps = (0,) + offsets(total)
    owner = jnp.zeros(shape, jnp.int32)
    strip = jnp.zeros(shape, jnp.int32)
    flip = jnp.zeros(shape, jnp.int32)
    for i in range(sides):
        here = rows // 2 == i
        held = jnp.maximum(conn_ref[0, i], 0)
        owner = jnp.where(here, held, owner)
        strip = jnp.where(here, conn_ref[1, i], strip)
        flip = jnp.where(here, conn_ref[2, i], flip)
        for d, offset in enumerate(steps):
            card = cards_ref[pl.ds(lax.rem(held + offset + total, total), 1), :]
            near_ref[d, pl.ds(2 * i, 1), :] = card
            near_ref[d, pl.ds(2 * i + 1, 1), :] = card

    def pick(array, index):
        return jnp.take_along_axis(array, index, axis=1)

    side = strip % 4
    base = strip - side
    at_end = jnp.where(rows % 2 == 0, 1 - flip, flip)
    across = side < 2
    other = jnp.where(across, 2 + at_end, at_end)
    odd = side % 2
    first = jnp.where(across, odd, at_end)
    second = jnp.where(across, at_end, odd)
    spread = 8 * jnp.minimum(lanes, 4)
    partner = near_ref[0]
    value = pick(partner, spread + base + 2 * first + 1 - second)
    link = CONN_LANE + 3 * (base + other)
    far_owner = pick(partner, link).astype(jnp.int32)
    far_strip = pick(partner, link + 1).astype(jnp.int32)
    far_flip = pick(partner, link + 2).astype(jnp.int32)
    far_card = partner
    for d, offset in enumerate(steps):
        if d:
            far_card = jnp.where(far_owner == lax.rem(owner + offset + total, total), near_ref[d], far_card)
    far_side = far_strip % 4
    far_base = far_strip - far_side
    point = jnp.where(far_flip == 1, 1 - odd, odd)
    far_across = far_side < 2
    far_odd = far_side % 2
    far_first = jnp.where(far_across, far_odd, point)
    far_second = jnp.where(far_across, point, far_odd)
    beyond = pick(far_card, spread + far_base + 2 * far_first + 1 - far_second)
    return jnp.where(far_owner >= 0, beyond - value, 0.0)


def last_kernel(
    fields_ref, inside_ref, density_ref, moduli_ref, diag_ref, cross_ref, left_ref, right_ref, own_ref, cards_ref,
    in0, in1, in2, in3, conn_ref, count_ref,
    final_out,
    table_ref, jump_ref, mine_ref, near_ref, scr_ref, turned_ref, corner_ref,
    cols_ref, rows_ref, xi_ref, eta_ref, rate_ref, final_ref, sems, *, total, scale,
):
    fields, slots, points, _ = fields_ref.shape
    sides = 4 * slots
    lanes = lane_ids((8, points))
    scr_ref[...] = jnp.zeros(scr_ref.shape, F32)

    for i in range(sides):
        table_ref[i] = own_ref[i]
    for k, in_ref in enumerate((in0, in1, in2, in3)):
        table_ref[sides + 2 * k] = in_ref[0]
        table_ref[sides + 2 * k + 1] = in_ref[1]
    weights = []
    partner_rates = []
    for i in range(sides):
        owner = conn_ref[0, i]
        strip = conn_ref[1, i]
        position = jnp.int32(0)
        for j in range(sides):
            if j != i:
                before = (conn_ref[0, j] == owner) & (conn_ref[1, j] < strip)
                position = position + before.astype(jnp.int32)
        place = strip
        for k, partner in enumerate(partners(lax.axis_index(PATCH_SUB), total)):
            place = jnp.where(owner == partner, sides + 2 * k + position, place)
        place = jnp.clip(place, 0, 2 * sides - 1)
        index = jnp.where(conn_ref[2, i] == 1, points - 1 - lanes, lanes)
        line = jnp.take_along_axis(table_ref[place, pl.ds(0, 8), :], index, axis=1)
        rate = jnp.take_along_axis(table_ref[place, pl.ds(8, 8), :], index, axis=1)
        weight = jnp.where(owner >= 0, scale, 0.0).astype(F32)
        jump = weight * (line - own_ref[i, pl.ds(0, 8), :])
        jump_ref[i] = jump
        weights.append(weight)
        partner_rates.append(rate - jump)
    turned_ref[...] = turn_jumps(jump_ref, scr_ref, fields, slots)

    for f in range(fields):
        for s in range(slots):
            rate_ref[f, s] = inside_ref[f, s] + column_part(turned_ref[...], 2 * (s * fields + f), points)
            for side, row in ((0, 0), (1, points - 1)):
                line = rate_ref[f, s, pl.ds(row, 1), :] + jump_ref[4 * s + side, pl.ds(f, 1), :]
                rate_ref[f, s, pl.ds(row, 1), :] = line
        derivatives(
            f, lambda s, f=f: rate_ref[f, s], left_ref, right_ref, cols_ref, rows_ref, xi_ref, eta_ref, slots, points
        )
    boundary_lines(rate_ref, mine_ref, 0, scr_ref, fields, slots, points)

    bound = jnp.max(cards_ref[...], axis=0, keepdims=True)
    bound = jnp.where(lane_ids(bound.shape) == PEAK_LANE, bound, 0.0)
    bound = jnp.max(bound, axis=1, keepdims=True)
    dt = CFL / (bound * (points - 1))
    half = 0.5 * dt * dt

    corner_ref[...] = jnp.zeros(corner_ref.shape, F32)
    corner_ref[pl.ds(0, 2 * sides), :] = corner_terms(cards_ref, conn_ref, near_ref, total, sides, points)
    corners = corner_ref[...].T[:8]
    for i in range(sides):
        partner = partner_rates[i] + scale * column_part(corners, 2 * i, points)
        jump_ref[i] = half * weights[i] * (partner - mine_ref[i])
    turned_ref[...] = turn_jumps(jump_ref, scr_ref, fields, slots)

    copies = []
    for s in range(slots):
        live = s < count_ref[0]
        for c in range(points // CHUNK):
            rows = pl.ds(c * CHUNK, CHUNK)
            parts = assemble(s, rows, density_ref, moduli_ref, diag_ref, cross_ref, xi_ref, eta_ref)
            for f in range(fields):
                value = fields_ref[f, s, rows, :] + dt * rate_ref[f, s, rows, :] + half * parts[f]
                value = value + column_part(turned_ref[rows, :], 2 * (s * fields + f), points)
                final_ref[f, s, rows, :] = jnp.where(live, value, 0.0)
        for f in range(fields):
            for side, row in ((0, 0), (1, points - 1)):
                line = final_ref[f, s, pl.ds(row, 1), :] + jump_ref[4 * s + side, pl.ds(f, 1), :]
                final_ref[f, s, pl.ds(row, 1), :] = jnp.where(live, line, 0.0)
            copy = pltpu.make_async_copy(final_ref.at[f, s], final_out.at[f, s], sems.at[s * fields + f])
            copy.start()
            copies.append(copy)
    for copy in copies:
        copy.wait()


def shards(fields, density, moduli, diag, cross, fc_extension, patch_count, connectivity):
    components, slots, points, _ = fields.shape
    total = lax.axis_size(PATCH_SUB)
    scale = PENALTY * (points - 1)
    sides = 4 * slots
    cont = fc_extension.shape[0]
    inner, outer = fourier_matrix(points, cont)
    links = connectivity.T

    def stay(x):
        return pltpu.with_memory_space_constraint(jnp.asarray(x), pltpu.HBM)

    def like(x):
        return jax.ShapeDtypeStruct(x.shape, x.dtype)

    box = jax.ShapeDtypeStruct((2, 16, points), F32)
    pair = jax.ShapeDtypeStruct((2 * points, 2 * points), BF16)
    square = pltpu.VMEM((points, points), F32)
    parts = pltpu.VMEM((components, 2 * points, 2 * points), BF16)
    grid = pltpu.VMEM(fields.shape, F32)

    (b0, b1, b2, b3, own, card, rate, left, right, fields, density, moduli, diag, cross, held) = pl.pallas_call(
        functools.partial(front_kernel, total=total),
        out_shape=[box] * 4
        + [
            jax.ShapeDtypeStruct((sides, 16, points), F32),
            jax.ShapeDtypeStruct((total, points), F32),
            like(fields),
            pair,
            pair,
        ]
        + [like(x) for x in (fields, density, moduli, diag, cross, links)],
        in_specs=[ANY] * 9 + [SMEM],
        out_specs=[VMEM] * 15,
        scratch_shapes=[
            square,
            pltpu.VMEM((points, cont), F32),
            pltpu.VMEM((fc_extension.shape[1], cont), F32),
            square,
            parts,
            parts,
            grid,
            grid,
            pltpu.SMEM(links.shape, jnp.int32),
            pltpu.SemaphoreType.DMA((9 + components,)),
        ],
        compiler_params=PARAMS,
        name="front",
    )(*[stay(x) for x in (fields, density, moduli, diag, cross, inner, outer, fc_extension.T, links)], patch_count)
    cards = lax.all_to_all(card, PATCH_SUB, 0, 0, tiled=True)
    arrived = [lax.ppermute(b, PATCH_SUB, route) for b, route in zip((b0, b1, b2, b3), routes(total))]
    line = pltpu.VMEM((sides, 8, points), F32)
    return pl.pallas_call(
        functools.partial(last_kernel, total=total, scale=scale),
        out_shape=like(fields),
        in_specs=[VMEM] * 14 + [SMEM] * 2,
        out_specs=ANY,
        scratch_shapes=[
            pltpu.VMEM((2 * sides, 16, points), F32),
            line,
            line,
            pltpu.VMEM((5, 2 * sides, points), F32),
            square,
            square,
            square,
            parts,
            parts,
            grid,
            grid,
            grid,
            grid,
            pltpu.SemaphoreType.DMA((components * slots,)),
        ],
        compiler_params=PARAMS,
        name="last",
    )(fields, rate, density, moduli, diag, cross, left, right, own, cards, *arrived, held, patch_count)


def solution(mesh):
    torus = Mesh(
        mesh.devices.reshape(4, 8, 4, mesh.shape["sub"]), ("patch_0", "patch_1", "patch_2", "sub")
    )
    return jax.shard_map(
        shards,
        mesh=torus,
        in_specs=(
            P(None, PATCH_SUB, None, None),
            P(PATCH_SUB, None, None),
            P(None, PATCH_SUB, None, None),
            P(None, PATCH_SUB, None, None),
            P(None, PATCH_SUB, None, None),
            P(),
            P(PATCH_SUB),
            P(PATCH_SUB, None),
        ),
        out_specs=P(None, PATCH_SUB, None, None),
        check_vma=False,
    )
```

```python
import functools

import jax
import jax.numpy as jnp
import numpy as np
from jax import lax
from jax.experimental import pallas as pl
from jax.experimental.pallas import tpu as pltpu
from jax.sharding import Mesh
from jax.sharding import PartitionSpec as P

PATCH_SUB = ("patch_0", "patch_1", "patch_2", "sub")

CFL = 0.5
PENALTY = 0.5
CHUNK = 16
F32 = jnp.float32
BF16 = jnp.bfloat16
VMEM = pl.BlockSpec(memory_space=pltpu.VMEM)
SMEM = pl.BlockSpec(memory_space=pltpu.SMEM)
ANY = pl.BlockSpec(memory_space=pltpu.HBM)
PARAMS = pltpu.CompilerParams(vmem_limit_bytes=14 * 1024 * 1024)
CONN_LANE = 40
PEAK_LANE = 64


def fourier_matrix(points, cont):
    length = points + cont
    delta = np.arange(points)[:, None] - np.arange(length)[None, :]
    safe = np.where(delta == 0, 1, delta)
    scale = np.pi * (points - 1) / length
    sign = np.where(delta % 2 == 0, 1.0, -1.0)
    full = np.where(delta == 0, 0.0, scale * sign / np.sin(np.pi * safe / length))
    return full[:, :points].astype(np.float32), full[:, points:].astype(np.float32)


def offsets(total):
    step = total // 2 + 1
    return (1, -1, step, -step)


ORDER = (3, 1, 2, 0)


def routes(total):
    return [
        [(i, (i + (offset if i % 2 == 0 else -offset)) % total) for i in range(total)]
        for offset in (offsets(total)[k] for k in ORDER)
    ]


def partners(me, total):
    sign = jnp.where(lax.rem(me, 2) == 0, 1, -1)
    return [lax.rem(me + sign * offsets(total)[k] + total, total) for k in ORDER]


def lane_ids(shape):
    return lax.broadcasted_iota(jnp.int32, shape, len(shape) - 1)


def split(value):
    high = value.astype(BF16)
    return high, (value - high.astype(F32)).astype(BF16)


def boundary_columns(load, scr_ref, fields, slots, points):
    lanes = lane_ids((points, points))
    columns = jnp.zeros((points, points), F32)
    for s in range(slots):
        for f in range(fields):
            at = 2 * (s * fields + f)
            columns = jnp.where((lanes == at) | (lanes == at + 1), pltpu.roll(load(f, s), at + 1, 1), columns)
    scr_ref[...] = columns.T


def boundary_lines(ref, own_ref, row, scr_ref, fields, slots, points):
    boundary_columns(lambda f, s: ref[f, s], scr_ref, fields, slots, points)
    for s in range(slots):
        for f in range(fields):
            own_ref[4 * s, pl.ds(row + f, 1), :] = ref[f, s, pl.ds(0, 1), :]
            own_ref[4 * s + 1, pl.ds(row + f, 1), :] = ref[f, s, pl.ds(points - 1, 1), :]
        base = 2 * s * fields
        own_ref[4 * s + 2, pl.ds(row, fields), :] = scr_ref[pl.ds(base + 1, fields, stride=2), :]
        own_ref[4 * s + 3, pl.ds(row, fields), :] = scr_ref[pl.ds(base, fields, stride=2), :]


def column_part(turned, at, points):
    moved = pltpu.roll(turned, points - 1 - at, 1)
    lanes = lane_ids(moved.shape)
    return jnp.where((lanes == 0) | (lanes == points - 1), moved, 0.0)


def turn_jumps(jump_ref, scr_ref, fields, slots):
    for s in range(slots):
        for f in range(fields):
            at = 2 * (s * fields + f)
            scr_ref[pl.ds(at + 1, 1), :] = jump_ref[4 * s + 2, pl.ds(f, 1), :]
            scr_ref[pl.ds(at, 1), :] = jump_ref[4 * s + 3, pl.ds(f, 1), :]
    return scr_ref[...].T


def derivatives(f, value_of, left_ref, right_ref, cols_ref, rows_ref, xi_ref, eta_ref, slots, points):
    for s in range(slots):
        high, low = split(value_of(s))
        cols_ref[f, pl.ds(0, points), pl.ds(s * points, points)] = high
        cols_ref[f, pl.ds(points, points), pl.ds(s * points, points)] = low
        rows_ref[f, pl.ds(s * points, points), pl.ds(0, points)] = high
        rows_ref[f, pl.ds(s * points, points), pl.ds(points, points)] = low
    got = jnp.dot(left_ref[...], cols_ref[f], preferred_element_type=F32)
    along = got[:points] + got[points:]
    for s in range(slots):
        xi_ref[f, s] = along[:, s * points : (s + 1) * points]
    got = jnp.dot(rows_ref[f], right_ref[...], preferred_element_type=F32)
    along = got[:, :points] + got[:, points:]
    for s in range(slots):
        eta_ref[f, s] = along[s * points : (s + 1) * points]


def assemble(s, rows, density_ref, moduli_ref, diag_ref, cross_ref, xi_ref, eta_ref):
    xi_x, eta_y = diag_ref[0, s, rows, :], diag_ref[1, s, rows, :]
    xi_y, eta_x = cross_ref[0, s, rows, :], cross_ref[1, s, rows, :]
    lame, shear = moduli_ref[0, s, rows, :], moduli_ref[1, s, rows, :]
    light = 1.0 / density_ref[s, rows, :]
    stiff = lame + 2.0 * shear

    def dx(f):
        return xi_x * xi_ref[f, s, rows, :] + eta_x * eta_ref[f, s, rows, :]

    def dy(f):
        return xi_y * xi_ref[f, s, rows, :] + eta_y * eta_ref[f, s, rows, :]

    one_x, two_y = dx(0), dy(1)
    return (
        (dx(2) + dy(4)) * light,
        (dx(4) + dy(3)) * light,
        stiff * one_x + lame * two_y,
        lame * one_x + stiff * two_y,
        shear * (dy(0) + dx(1)),
    )


def build_matrices(inner, outer, ext, match, left_ref, right_ref):
    points = inner.shape[0]
    folded = lax.dot_general(
        outer, ext, (((1,), (1,)), ((), ())), precision=lax.Precision.HIGHEST, preferred_element_type=F32
    )
    full = inner + pltpu.roll(folded, points - match, 1)
    zero = jnp.zeros((points, points), BF16)
    first, second = pl.ds(0, points), pl.ds(points, points)
    high, low = split(full)
    left_ref[first, first] = high
    left_ref[first, second] = high
    left_ref[second, first] = low
    left_ref[second, second] = zero
    high, low = split(full.T)
    right_ref[first, first] = high
    right_ref[second, first] = high
    right_ref[first, second] = low
    right_ref[second, second] = zero


def front_kernel(
    fields_in, density_in, moduli_in, diag_in, cross_in, inner_in, outer_in, ext_in, conn_in, count_ref,
    out0, out1, out2, out3, own_ref, card_ref, rate_ref, left_ref, right_ref,
    fields_ref, density_ref, moduli_ref, diag_ref, cross_ref, links_ref,
    inner_ref, outer_ref, ext_ref, scr_ref, cols_ref, rows_ref, xi_ref, eta_ref, conn_ref, rows_out_ref, sems, *, total,
):
    fields, slots, points, _ = fields_ref.shape
    sides = 4 * slots

    ext_ref[...] = jnp.zeros(ext_ref.shape, F32)

    def fetch(source, target, at):
        copy = pltpu.make_async_copy(source, target, sems.at[at])
        copy.start()
        return copy

    small = [fetch(a, b, i) for i, (a, b) in enumerate(((inner_in, inner_ref), (outer_in, outer_ref), (ext_in, ext_ref.at[pl.ds(0, ext_in.shape[0])])))]
    coefs = [
        fetch(a, b, 3 + fields + i)
        for i, (a, b) in enumerate(
            ((density_in, density_ref), (moduli_in, moduli_ref), (diag_in, diag_ref), (cross_in, cross_ref))
        )
    ]
    large = [fetch(fields_in.at[f], fields_ref.at[f], 3 + f) for f in range(fields)]
    links = [fetch(conn_in, conn_ref, 7 + fields), fetch(conn_in, links_ref, 8 + fields)]
    for copy in small:
        copy.wait()
    build_matrices(inner_ref[...], outer_ref[...], ext_ref[...], ext_in.shape[0] // 2, left_ref, right_ref)
    for copy in coefs + links:
        copy.wait()

    peak = jnp.zeros((8, points), F32)
    for s in range(slots):
        live = s < count_ref[0]
        for c in range(points // CHUNK):
            rows = pl.ds(c * CHUNK, CHUNK)
            stiff = moduli_ref[0, s, rows, :] + 2.0 * moduli_ref[1, s, rows, :]
            xi_x, eta_y = diag_ref[0, s, rows, :], diag_ref[1, s, rows, :]
            xi_y, eta_x = cross_ref[0, s, rows, :], cross_ref[1, s, rows, :]
            speed = jnp.sqrt(stiff / density_ref[s, rows, :]) * (
                jnp.sqrt(xi_x * xi_x + xi_y * xi_y) + jnp.sqrt(eta_x * eta_x + eta_y * eta_y)
            )
            speed = jnp.where(live, speed, 0.0)
            for r in range(CHUNK // 8):
                peak = jnp.maximum(peak, speed[8 * r : 8 * r + 8])
    peak = jnp.max(jnp.max(peak, axis=0, keepdims=True), axis=1, keepdims=True)

    for copy in large:
        copy.wait()
    boundary_lines(fields_ref, own_ref, 0, scr_ref, fields, slots, points)
    lanes = lane_ids((8, points))
    corners = jnp.zeros((8, points), F32)
    for s in range(slots):
        for a in range(2):
            k = 4 * s + 2 * a
            moved = pltpu.roll(own_ref[4 * s + a, pl.ds(0, 8), :], k + 1, 1)
            corners = jnp.where((lanes == k) | (lanes == k + 1), moved, corners)
    scr_ref[pl.ds(0, 8), :] = corners
    lane = lane_ids((1, points))
    card = jnp.where(lane == PEAK_LANE, peak, 0.0)
    for f in range(fields):
        moved = pltpu.roll(scr_ref[pl.ds(f, 1), :], 8 * f, 1)
        card = jnp.where((lane >= 8 * f) & (lane < 8 * f + sides), moved, card)
    for i in range(sides):
        for c in range(3):
            card = jnp.where(lane == CONN_LANE + 3 * i + c, conn_ref[c, i].astype(F32), card)
    rows_out_ref[...] = jnp.broadcast_to(card, rows_out_ref.shape)
    sent = fetch(rows_out_ref, card_ref, 9 + fields)

    for f in range(fields):
        derivatives(
            f, lambda s, f=f: fields_ref[f, s], left_ref, right_ref, cols_ref, rows_ref, xi_ref, eta_ref, slots, points
        )
    for s in range(slots):
        for c in range(points // CHUNK):
            rows = pl.ds(c * CHUNK, CHUNK)
            parts = assemble(s, rows, density_ref, moduli_ref, diag_ref, cross_ref, xi_ref, eta_ref)
            for f in range(fields):
                rate_ref[f, s, rows, :] = parts[f]
    boundary_lines(rate_ref, own_ref, 8, scr_ref, fields, slots, points)

    for partner, out_ref in zip(partners(lax.axis_index(PATCH_SUB), total), (out0, out1, out2, out3)):
        first = jnp.int32(0)
        second = jnp.int32(0)
        count = jnp.int32(0)
        for i in range(sides):
            match = conn_ref[0, i] == partner
            first = jnp.where(match & (count == 0), i, first)
            second = jnp.where(match & (count == 1), i, second)
            count = count + match.astype(jnp.int32)
        out_ref[0] = own_ref[first]
        out_ref[1] = own_ref[second]
    sent.wait()


def corner_terms(cards_ref, conn_ref, near_ref, total, sides, points):
    shape = (2 * sides, points)
    rows = lax.broadcasted_iota(jnp.int32, shape, 0)
    lanes = lane_ids(shape)
    steps = (0,) + offsets(total)
    owner = jnp.zeros(shape, jnp.int32)
    strip = jnp.zeros(shape, jnp.int32)
    flip = jnp.zeros(shape, jnp.int32)
    for i in range(sides):
        here = rows // 2 == i
        held = jnp.maximum(conn_ref[0, i], 0)
        owner = jnp.where(here, held, owner)
        strip = jnp.where(here, conn_ref[1, i], strip)
        flip = jnp.where(here, conn_ref[2, i], flip)
        for d, offset in enumerate(steps):
            card = cards_ref[pl.ds(lax.rem(held + offset + total, total), 1), :]
            near_ref[d, pl.ds(2 * i, 1), :] = card
            near_ref[d, pl.ds(2 * i + 1, 1), :] = card

    def pick(array, index):
        return jnp.take_along_axis(array, index, axis=1)

    side = strip % 4
    base = strip - side
    at_end = jnp.where(rows % 2 == 0, 1 - flip, flip)
    across = side < 2
    other = jnp.where(across, 2 + at_end, at_end)
    odd = side % 2
    first = jnp.where(across, odd, at_end)
    second = jnp.where(across, at_end, odd)
    spread = 8 * jnp.minimum(lanes, 4)
    partner = near_ref[0]
    value = pick(partner, spread + base + 2 * first + 1 - second)
    link = CONN_LANE + 3 * (base + other)
    far_owner = pick(partner, link).astype(jnp.int32)
    far_strip = pick(partner, link + 1).astype(jnp.int32)
    far_flip = pick(partner, link + 2).astype(jnp.int32)
    far_card = partner
    for d, offset in enumerate(steps):
        if d:
            far_card = jnp.where(far_owner == lax.rem(owner + offset + total, total), near_ref[d], far_card)
    far_side = far_strip % 4
    far_base = far_strip - far_side
    point = jnp.where(far_flip == 1, 1 - odd, odd)
    far_across = far_side < 2
    far_odd = far_side % 2
    far_first = jnp.where(far_across, far_odd, point)
    far_second = jnp.where(far_across, point, far_odd)
    beyond = pick(far_card, spread + far_base + 2 * far_first + 1 - far_second)
    return jnp.where(far_owner >= 0, beyond - value, 0.0)


def last_kernel(
    fields_ref, inside_ref, density_ref, moduli_ref, diag_ref, cross_ref, left_ref, right_ref, own_ref, cards_ref,
    in0, in1, in2, in3, conn_ref, count_ref,
    final_out,
    table_ref, jump_ref, mine_ref, near_ref, scr_ref, turned_ref, corner_ref,
    cols_ref, rows_ref, xi_ref, eta_ref, rate_ref, final_ref, sems, *, total, scale,
):
    fields, slots, points, _ = fields_ref.shape
    sides = 4 * slots
    lanes = lane_ids((8, points))
    scr_ref[...] = jnp.zeros(scr_ref.shape, F32)

    for i in range(sides):
        table_ref[i] = own_ref[i]
    for k, in_ref in enumerate((in0, in1, in2, in3)):
        table_ref[sides + 2 * k] = in_ref[0]
        table_ref[sides + 2 * k + 1] = in_ref[1]
    weights = []
    partner_rates = []
    for i in range(sides):
        owner = conn_ref[0, i]
        strip = conn_ref[1, i]
        position = jnp.int32(0)
        for j in range(sides):
            if j != i:
                before = (conn_ref[0, j] == owner) & (conn_ref[1, j] < strip)
                position = position + before.astype(jnp.int32)
        place = strip
        for k, partner in enumerate(partners(lax.axis_index(PATCH_SUB), total)):
            place = jnp.where(owner == partner, sides + 2 * k + position, place)
        place = jnp.clip(place, 0, 2 * sides - 1)
        index = jnp.where(conn_ref[2, i] == 1, points - 1 - lanes, lanes)
        line = jnp.take_along_axis(table_ref[place, pl.ds(0, 8), :], index, axis=1)
        rate = jnp.take_along_axis(table_ref[place, pl.ds(8, 8), :], index, axis=1)
        weight = jnp.where(owner >= 0, scale, 0.0).astype(F32)
        jump = weight * (line - own_ref[i, pl.ds(0, 8), :])
        jump_ref[i] = jump
        weights.append(weight)
        partner_rates.append(rate - jump)
    turned_ref[...] = turn_jumps(jump_ref, scr_ref, fields, slots)

    for f in range(fields):
        for s in range(slots):
            rate_ref[f, s] = inside_ref[f, s] + column_part(turned_ref[...], 2 * (s * fields + f), points)
            for side, row in ((0, 0), (1, points - 1)):
                line = rate_ref[f, s, pl.ds(row, 1), :] + jump_ref[4 * s + side, pl.ds(f, 1), :]
                rate_ref[f, s, pl.ds(row, 1), :] = line
        derivatives(
            f, lambda s, f=f: rate_ref[f, s], left_ref, right_ref, cols_ref, rows_ref, xi_ref, eta_ref, slots, points
        )
    boundary_lines(rate_ref, mine_ref, 0, scr_ref, fields, slots, points)

    bound = jnp.max(cards_ref[...], axis=0, keepdims=True)
    bound = jnp.where(lane_ids(bound.shape) == PEAK_LANE, bound, 0.0)
    bound = jnp.max(bound, axis=1, keepdims=True)
    dt = CFL / (bound * (points - 1))
    half = 0.5 * dt * dt

    corner_ref[...] = jnp.zeros(corner_ref.shape, F32)
    corner_ref[pl.ds(0, 2 * sides), :] = corner_terms(cards_ref, conn_ref, near_ref, total, sides, points)
    corners = corner_ref[...].T[:8]
    for i in range(sides):
        partner = partner_rates[i] + scale * column_part(corners, 2 * i, points)
        jump_ref[i] = half * weights[i] * (partner - mine_ref[i])
    turned_ref[...] = turn_jumps(jump_ref, scr_ref, fields, slots)

    copies = []
    for s in range(slots):
        live = s < count_ref[0]
        for c in range(points // CHUNK):
            rows = pl.ds(c * CHUNK, CHUNK)
            parts = assemble(s, rows, density_ref, moduli_ref, diag_ref, cross_ref, xi_ref, eta_ref)
            for f in range(fields):
                value = fields_ref[f, s, rows, :] + dt * rate_ref[f, s, rows, :] + half * parts[f]
                value = value + column_part(turned_ref[rows, :], 2 * (s * fields + f), points)
                final_ref[f, s, rows, :] = jnp.where(live, value, 0.0)
        for f in range(fields):
            for side, row in ((0, 0), (1, points - 1)):
                line = final_ref[f, s, pl.ds(row, 1), :] + jump_ref[4 * s + side, pl.ds(f, 1), :]
                final_ref[f, s, pl.ds(row, 1), :] = jnp.where(live, line, 0.0)
            copy = pltpu.make_async_copy(final_ref.at[f, s], final_out.at[f, s], sems.at[s * fields + f])
            copy.start()
            copies.append(copy)
    for copy in copies:
        copy.wait()


def shards(fields, density, moduli, diag, cross, fc_extension, patch_count, connectivity):
    components, slots, points, _ = fields.shape
    total = lax.axis_size(PATCH_SUB)
    scale = PENALTY * (points - 1)
    sides = 4 * slots
    cont = fc_extension.shape[0]
    inner, outer = fourier_matrix(points, cont)
    links = connectivity.T

    def stay(x):
        return pltpu.with_memory_space_constraint(jnp.asarray(x), pltpu.HBM)

    def like(x):
        return jax.ShapeDtypeStruct(x.shape, x.dtype)

    box = jax.ShapeDtypeStruct((2, 16, points), F32)
    pair = jax.ShapeDtypeStruct((2 * points, 2 * points), BF16)
    square = pltpu.VMEM((points, points), F32)
    parts = pltpu.VMEM((components, 2 * points, 2 * points), BF16)
    grid = pltpu.VMEM(fields.shape, F32)

    (b0, b1, b2, b3, own, card, rate, left, right, fields, density, moduli, diag, cross, held) = pl.pallas_call(
        functools.partial(front_kernel, total=total),
        out_shape=[box] * 4
        + [
            jax.ShapeDtypeStruct((sides, 16, points), F32),
            jax.ShapeDtypeStruct((total, points), F32),
            like(fields),
            pair,
            pair,
        ]
        + [like(x) for x in (fields, density, moduli, diag, cross, links)],
        in_specs=[ANY] * 9 + [SMEM],
        out_specs=[VMEM] * 5 + [ANY] + [VMEM] * 9,
        scratch_shapes=[
            square,
            pltpu.VMEM((points, cont), F32),
            pltpu.VMEM((points, cont), F32),
            square,
            parts,
            parts,
            grid,
            grid,
            pltpu.SMEM(links.shape, jnp.int32),
            pltpu.VMEM((total, points), F32),
            pltpu.SemaphoreType.DMA((10 + components,)),
        ],
        compiler_params=PARAMS,
        name="front",
    )(*[stay(x) for x in (fields, density, moduli, diag, cross, inner, outer, fc_extension.T, links)], patch_count)
    cards = lax.all_to_all(card, PATCH_SUB, 0, 0, tiled=True)
    arrived = [lax.ppermute(b, PATCH_SUB, route) for b, route in zip((b0, b1, b2, b3), routes(total))]
    line = pltpu.VMEM((sides, 8, points), F32)
    return pl.pallas_call(
        functools.partial(last_kernel, total=total, scale=scale),
        out_shape=like(fields),
        in_specs=[VMEM] * 14 + [SMEM] * 2,
        out_specs=ANY,
        scratch_shapes=[
            pltpu.VMEM((2 * sides, 16, points), F32),
            line,
            line,
            pltpu.VMEM((5, 2 * sides, points), F32),
            square,
            square,
            square,
            parts,
            parts,
            grid,
            grid,
            grid,
            grid,
            pltpu.SemaphoreType.DMA((components * slots,)),
        ],
        compiler_params=PARAMS,
        name="last",
    )(fields, rate, density, moduli, diag, cross, left, right, own, cards, *arrived, held, patch_count)


def solution(mesh):
    torus = Mesh(
        mesh.devices.reshape(4, 8, 4, mesh.shape["sub"]), ("patch_0", "patch_1", "patch_2", "sub")
    )
    return jax.shard_map(
        shards,
        mesh=torus,
        in_specs=(
            P(None, PATCH_SUB, None, None),
            P(PATCH_SUB, None, None),
            P(None, PATCH_SUB, None, None),
            P(None, PATCH_SUB, None, None),
            P(None, PATCH_SUB, None, None),
            P(),
            P(PATCH_SUB),
            P(PATCH_SUB, None),
        ),
        out_specs=P(None, PATCH_SUB, None, None),
        check_vma=False,
    )
```

```python
import functools

import jax
import jax.numpy as jnp
import numpy as np
from jax import lax
from jax.experimental import pallas as pl
from jax.experimental.pallas import tpu as pltpu
from jax.sharding import Mesh
from jax.sharding import PartitionSpec as P

PATCH_SUB = ("patch_0", "patch_1", "patch_2", "sub")

CFL = 0.5
PENALTY = 0.5
CHUNK = 16
F32 = jnp.float32
BF16 = jnp.bfloat16
VMEM = pl.BlockSpec(memory_space=pltpu.VMEM)
SMEM = pl.BlockSpec(memory_space=pltpu.SMEM)
ANY = pl.BlockSpec(memory_space=pltpu.HBM)
PARAMS = pltpu.CompilerParams(vmem_limit_bytes=14 * 1024 * 1024)
CONN_LANE = 40
PEAK_LANE = 64


def fourier_matrix(points, cont):
    length = points + cont
    delta = np.arange(points)[:, None] - np.arange(length)[None, :]
    safe = np.where(delta == 0, 1, delta)
    scale = np.pi * (points - 1) / length
    sign = np.where(delta % 2 == 0, 1.0, -1.0)
    full = np.where(delta == 0, 0.0, scale * sign / np.sin(np.pi * safe / length))
    return full[:, :points].astype(np.float32), full[:, points:].astype(np.float32)


def offsets(total):
    step = total // 2 + 1
    return (1, -1, step, -step)


ORDER = (3, 1, 2, 0)


def routes(total):
    return [
        [(i, (i + (offset if i % 2 == 0 else -offset)) % total) for i in range(total)]
        for offset in (offsets(total)[k] for k in ORDER)
    ]


def partners(me, total):
    sign = jnp.where(lax.rem(me, 2) == 0, 1, -1)
    return [lax.rem(me + sign * offsets(total)[k] + total, total) for k in ORDER]


def lane_ids(shape):
    return lax.broadcasted_iota(jnp.int32, shape, len(shape) - 1)


def split(value):
    high = value.astype(BF16)
    return high, (value - high.astype(F32)).astype(BF16)


def boundary_columns(load, scr_ref, fields, slots, points):
    lanes = lane_ids((points, points))
    columns = jnp.zeros((points, points), F32)
    for s in range(slots):
        for f in range(fields):
            at = 2 * (s * fields + f)
            columns = jnp.where((lanes == at) | (lanes == at + 1), pltpu.roll(load(f, s), at + 1, 1), columns)
    scr_ref[...] = columns.T


def boundary_lines(ref, own_ref, row, scr_ref, fields, slots, points):
    boundary_columns(lambda f, s: ref[f, s], scr_ref, fields, slots, points)
    for s in range(slots):
        for f in range(fields):
            own_ref[4 * s, pl.ds(row + f, 1), :] = ref[f, s, pl.ds(0, 1), :]
            own_ref[4 * s + 1, pl.ds(row + f, 1), :] = ref[f, s, pl.ds(points - 1, 1), :]
        base = 2 * s * fields
        own_ref[4 * s + 2, pl.ds(row, fields), :] = scr_ref[pl.ds(base + 1, fields, stride=2), :]
        own_ref[4 * s + 3, pl.ds(row, fields), :] = scr_ref[pl.ds(base, fields, stride=2), :]


def column_part(turned, at, points):
    moved = pltpu.roll(turned, points - 1 - at, 1)
    lanes = lane_ids(moved.shape)
    return jnp.where((lanes == 0) | (lanes == points - 1), moved, 0.0)


def turn_jumps(jump_ref, scr_ref, fields, slots):
    for s in range(slots):
        for f in range(fields):
            at = 2 * (s * fields + f)
            scr_ref[pl.ds(at + 1, 1), :] = jump_ref[4 * s + 2, pl.ds(f, 1), :]
            scr_ref[pl.ds(at, 1), :] = jump_ref[4 * s + 3, pl.ds(f, 1), :]
    return scr_ref[...].T


def derivatives(f, value_of, left_ref, right_ref, cols_ref, rows_ref, xi_ref, eta_ref, slots, points):
    for s in range(slots):
        high, low = split(value_of(s))
        cols_ref[f, pl.ds(0, points), pl.ds(s * points, points)] = high
        cols_ref[f, pl.ds(points, points), pl.ds(s * points, points)] = low
        rows_ref[f, pl.ds(s * points, points), pl.ds(0, points)] = high
        rows_ref[f, pl.ds(s * points, points), pl.ds(points, points)] = low
    got = jnp.dot(left_ref[...], cols_ref[f], preferred_element_type=F32)
    along = got[:points] + got[points:]
    for s in range(slots):
        xi_ref[f, s] = along[:, s * points : (s + 1) * points]
    got = jnp.dot(rows_ref[f], right_ref[...], preferred_element_type=F32)
    along = got[:, :points] + got[:, points:]
    for s in range(slots):
        eta_ref[f, s] = along[s * points : (s + 1) * points]


def assemble(s, rows, density_ref, moduli_ref, diag_ref, cross_ref, xi_ref, eta_ref):
    xi_x, eta_y = diag_ref[0, s, rows, :], diag_ref[1, s, rows, :]
    xi_y, eta_x = cross_ref[0, s, rows, :], cross_ref[1, s, rows, :]
    lame, shear = moduli_ref[0, s, rows, :], moduli_ref[1, s, rows, :]
    light = 1.0 / density_ref[s, rows, :]
    stiff = lame + 2.0 * shear

    def dx(f):
        return xi_x * xi_ref[f, s, rows, :] + eta_x * eta_ref[f, s, rows, :]

    def dy(f):
        return xi_y * xi_ref[f, s, rows, :] + eta_y * eta_ref[f, s, rows, :]

    one_x, two_y = dx(0), dy(1)
    return (
        (dx(2) + dy(4)) * light,
        (dx(4) + dy(3)) * light,
        stiff * one_x + lame * two_y,
        lame * one_x + stiff * two_y,
        shear * (dy(0) + dx(1)),
    )


def build_matrices(inner, outer, ext, match, left_ref, right_ref):
    points = inner.shape[0]
    folded = lax.dot_general(
        outer, ext, (((1,), (1,)), ((), ())), precision=lax.Precision.HIGHEST, preferred_element_type=F32
    )
    full = inner + pltpu.roll(folded, points - match, 1)
    zero = jnp.zeros((points, points), BF16)
    first, second = pl.ds(0, points), pl.ds(points, points)
    high, low = split(full)
    left_ref[first, first] = high
    left_ref[first, second] = high
    left_ref[second, first] = low
    left_ref[second, second] = zero
    high, low = split(full.T)
    right_ref[first, first] = high
    right_ref[second, first] = high
    right_ref[first, second] = low
    right_ref[second, second] = zero


def front_kernel(
    fields_in, density_in, moduli_in, diag_in, cross_in, inner_in, outer_in, ext_in, conn_in, count_ref,
    out0, out1, out2, out3, own_ref, card_ref, rate_ref, left_ref, right_ref,
    fields_ref, density_ref, moduli_ref, diag_ref, cross_ref, links_ref,
    inner_ref, outer_ref, ext_ref, scr_ref, cols_ref, rows_ref, xi_ref, eta_ref, conn_ref, rows_out_ref, sems, *, total,
):
    fields, slots, points, _ = fields_ref.shape
    sides = 4 * slots

    ext_ref[...] = jnp.zeros(ext_ref.shape, F32)

    def fetch(source, target, at):
        copy = pltpu.make_async_copy(source, target, sems.at[at])
        copy.start()
        return copy

    small = [fetch(a, b, i) for i, (a, b) in enumerate(((inner_in, inner_ref), (outer_in, outer_ref), (ext_in, ext_ref.at[pl.ds(0, ext_in.shape[0])])))]
    coefs = [
        fetch(a, b, 3 + fields + i)
        for i, (a, b) in enumerate(
            ((density_in, density_ref), (moduli_in, moduli_ref), (diag_in, diag_ref), (cross_in, cross_ref))
        )
    ]
    large = [fetch(fields_in.at[f], fields_ref.at[f], 3 + f) for f in range(fields)]
    links = [fetch(conn_in, conn_ref, 7 + fields), fetch(conn_in, links_ref, 8 + fields)]
    for copy in small:
        copy.wait()
    build_matrices(inner_ref[...], outer_ref[...], ext_ref[...], ext_in.shape[0] // 2, left_ref, right_ref)
    for copy in coefs + links:
        copy.wait()

    peak = jnp.zeros((8, points), F32)
    for s in range(slots):
        live = s < count_ref[0]
        for c in range(points // CHUNK):
            rows = pl.ds(c * CHUNK, CHUNK)
            stiff = moduli_ref[0, s, rows, :] + 2.0 * moduli_ref[1, s, rows, :]
            xi_x, eta_y = diag_ref[0, s, rows, :], diag_ref[1, s, rows, :]
            xi_y, eta_x = cross_ref[0, s, rows, :], cross_ref[1, s, rows, :]
            speed = jnp.sqrt(stiff / density_ref[s, rows, :]) * (
                jnp.sqrt(xi_x * xi_x + xi_y * xi_y) + jnp.sqrt(eta_x * eta_x + eta_y * eta_y)
            )
            speed = jnp.where(live, speed, 0.0)
            for r in range(CHUNK // 8):
                peak = jnp.maximum(peak, speed[8 * r : 8 * r + 8])
    peak = jnp.max(jnp.max(peak, axis=0, keepdims=True), axis=1, keepdims=True)

    for copy in large:
        copy.wait()
    boundary_lines(fields_ref, own_ref, 0, scr_ref, fields, slots, points)
    lanes = lane_ids((8, points))
    corners = jnp.zeros((8, points), F32)
    for s in range(slots):
        for a in range(2):
            k = 4 * s + 2 * a
            moved = pltpu.roll(own_ref[4 * s + a, pl.ds(0, 8), :], k + 1, 1)
            corners = jnp.where((lanes == k) | (lanes == k + 1), moved, corners)
    scr_ref[pl.ds(0, 8), :] = corners
    lane = lane_ids((1, points))
    card = jnp.where(lane == PEAK_LANE, peak, 0.0)
    for f in range(fields):
        moved = pltpu.roll(scr_ref[pl.ds(f, 1), :], 8 * f, 1)
        card = jnp.where((lane >= 8 * f) & (lane < 8 * f + sides), moved, card)
    for i in range(sides):
        for c in range(3):
            card = jnp.where(lane == CONN_LANE + 3 * i + c, conn_ref[c, i].astype(F32), card)
    rows_out_ref[...] = jnp.broadcast_to(card, rows_out_ref.shape)
    sent = fetch(rows_out_ref, card_ref, 9 + fields)

    for f in range(fields):
        derivatives(
            f, lambda s, f=f: fields_ref[f, s], left_ref, right_ref, cols_ref, rows_ref, xi_ref, eta_ref, slots, points
        )
    for s in range(slots):
        for c in range(points // CHUNK):
            rows = pl.ds(c * CHUNK, CHUNK)
            parts = assemble(s, rows, density_ref, moduli_ref, diag_ref, cross_ref, xi_ref, eta_ref)
            for f in range(fields):
                rate_ref[f, s, rows, :] = parts[f]
    boundary_lines(rate_ref, own_ref, 8, scr_ref, fields, slots, points)

    for partner, out_ref in zip(partners(lax.axis_index(PATCH_SUB), total), (out0, out1, out2, out3)):
        first = jnp.int32(0)
        second = jnp.int32(0)
        count = jnp.int32(0)
        for i in range(sides):
            match = conn_ref[0, i] == partner
            first = jnp.where(match & (count == 0), i, first)
            second = jnp.where(match & (count == 1), i, second)
            count = count + match.astype(jnp.int32)
        out_ref[0] = own_ref[first]
        out_ref[1] = own_ref[second]
    sent.wait()


def corner_terms(cards_ref, conn_ref, near_ref, total, sides, points):
    shape = (2 * sides, points)
    rows = lax.broadcasted_iota(jnp.int32, shape, 0)
    lanes = lane_ids(shape)
    steps = (0,) + offsets(total)
    owner = jnp.zeros(shape, jnp.int32)
    strip = jnp.zeros(shape, jnp.int32)
    flip = jnp.zeros(shape, jnp.int32)
    for i in range(sides):
        here = rows // 2 == i
        held = jnp.maximum(conn_ref[0, i], 0)
        owner = jnp.where(here, held, owner)
        strip = jnp.where(here, conn_ref[1, i], strip)
        flip = jnp.where(here, conn_ref[2, i], flip)
        for d, offset in enumerate(steps):
            card = cards_ref[pl.ds(lax.rem(held + offset + total, total), 1), :]
            near_ref[d, pl.ds(2 * i, 1), :] = card
            near_ref[d, pl.ds(2 * i + 1, 1), :] = card

    def pick(array, index):
        return jnp.take_along_axis(array, index, axis=1)

    side = strip % 4
    base = strip - side
    at_end = jnp.where(rows % 2 == 0, 1 - flip, flip)
    across = side < 2
    other = jnp.where(across, 2 + at_end, at_end)
    odd = side % 2
    first = jnp.where(across, odd, at_end)
    second = jnp.where(across, at_end, odd)
    spread = 8 * jnp.minimum(lanes, 4)
    partner = near_ref[0]
    value = pick(partner, spread + base + 2 * first + 1 - second)
    link = CONN_LANE + 3 * (base + other)
    far_owner = pick(partner, link).astype(jnp.int32)
    far_strip = pick(partner, link + 1).astype(jnp.int32)
    far_flip = pick(partner, link + 2).astype(jnp.int32)
    far_card = partner
    for d, offset in enumerate(steps):
        if d:
            far_card = jnp.where(far_owner == lax.rem(owner + offset + total, total), near_ref[d], far_card)
    far_side = far_strip % 4
    far_base = far_strip - far_side
    point = jnp.where(far_flip == 1, 1 - odd, odd)
    far_across = far_side < 2
    far_odd = far_side % 2
    far_first = jnp.where(far_across, far_odd, point)
    far_second = jnp.where(far_across, point, far_odd)
    beyond = pick(far_card, spread + far_base + 2 * far_first + 1 - far_second)
    return jnp.where(far_owner >= 0, beyond - value, 0.0)


def last_kernel(
    fields_ref, inside_ref, density_ref, moduli_ref, diag_ref, cross_ref, left_ref, right_ref, own_ref, cards_ref,
    in0, in1, in2, in3, conn_ref, count_ref,
    final_out,
    table_ref, jump_ref, mine_ref, near_ref, scr_ref, turned_ref, corner_ref,
    cols_ref, rows_ref, xi_ref, eta_ref, rate_ref, final_ref, sems, *, total, scale,
):
    fields, slots, points, _ = fields_ref.shape
    sides = 4 * slots
    lanes = lane_ids((8, points))
    scr_ref[...] = jnp.zeros(scr_ref.shape, F32)

    corner_ref[...] = jnp.zeros(corner_ref.shape, F32)
    corner_ref[pl.ds(0, 2 * sides), :] = corner_terms(cards_ref, conn_ref, near_ref, total, sides, points)
    for i in range(sides):
        table_ref[i] = own_ref[i]
    for k, in_ref in enumerate((in0, in1, in2, in3)):
        table_ref[sides + 2 * k] = in_ref[0]
        table_ref[sides + 2 * k + 1] = in_ref[1]
    weights = []
    partner_rates = []
    for i in range(sides):
        owner = conn_ref[0, i]
        strip = conn_ref[1, i]
        position = jnp.int32(0)
        for j in range(sides):
            if j != i:
                before = (conn_ref[0, j] == owner) & (conn_ref[1, j] < strip)
                position = position + before.astype(jnp.int32)
        place = strip
        for k, partner in enumerate(partners(lax.axis_index(PATCH_SUB), total)):
            place = jnp.where(owner == partner, sides + 2 * k + position, place)
        place = jnp.clip(place, 0, 2 * sides - 1)
        index = jnp.where(conn_ref[2, i] == 1, points - 1 - lanes, lanes)
        line = jnp.take_along_axis(table_ref[place, pl.ds(0, 8), :], index, axis=1)
        rate = jnp.take_along_axis(table_ref[place, pl.ds(8, 8), :], index, axis=1)
        weight = jnp.where(owner >= 0, scale, 0.0).astype(F32)
        jump = weight * (line - own_ref[i, pl.ds(0, 8), :])
        jump_ref[i] = jump
        weights.append(weight)
        partner_rates.append(rate - jump)
    turned_ref[...] = turn_jumps(jump_ref, scr_ref, fields, slots)

    for f in range(fields):
        for s in range(slots):
            rate_ref[f, s] = inside_ref[f, s] + column_part(turned_ref[...], 2 * (s * fields + f), points)
            for side, row in ((0, 0), (1, points - 1)):
                line = rate_ref[f, s, pl.ds(row, 1), :] + jump_ref[4 * s + side, pl.ds(f, 1), :]
                rate_ref[f, s, pl.ds(row, 1), :] = line
        derivatives(
            f, lambda s, f=f: rate_ref[f, s], left_ref, right_ref, cols_ref, rows_ref, xi_ref, eta_ref, slots, points
        )
    boundary_lines(rate_ref, mine_ref, 0, scr_ref, fields, slots, points)

    bound = jnp.max(cards_ref[...], axis=0, keepdims=True)
    bound = jnp.where(lane_ids(bound.shape) == PEAK_LANE, bound, 0.0)
    bound = jnp.max(bound, axis=1, keepdims=True)
    dt = CFL / (bound * (points - 1))
    half = 0.5 * dt * dt

    corners = corner_ref[...].T[:8]
    for i in range(sides):
        partner = partner_rates[i] + scale * column_part(corners, 2 * i, points)
        jump_ref[i] = half * weights[i] * (partner - mine_ref[i])
    turned_ref[...] = turn_jumps(jump_ref, scr_ref, fields, slots)

    copies = []
    for s in range(slots):
        live = s < count_ref[0]
        for c in range(points // CHUNK):
            rows = pl.ds(c * CHUNK, CHUNK)
            parts = assemble(s, rows, density_ref, moduli_ref, diag_ref, cross_ref, xi_ref, eta_ref)
            for f in range(fields):
                value = fields_ref[f, s, rows, :] + dt * rate_ref[f, s, rows, :] + half * parts[f]
                value = value + column_part(turned_ref[rows, :], 2 * (s * fields + f), points)
                final_ref[f, s, rows, :] = jnp.where(live, value, 0.0)
        for f in range(fields):
            for side, row in ((0, 0), (1, points - 1)):
                line = final_ref[f, s, pl.ds(row, 1), :] + jump_ref[4 * s + side, pl.ds(f, 1), :]
                final_ref[f, s, pl.ds(row, 1), :] = jnp.where(live, line, 0.0)
            copy = pltpu.make_async_copy(final_ref.at[f, s], final_out.at[f, s], sems.at[s * fields + f])
            copy.start()
            copies.append(copy)
    for copy in copies:
        copy.wait()


def shards(fields, density, moduli, diag, cross, fc_extension, patch_count, connectivity):
    components, slots, points, _ = fields.shape
    total = lax.axis_size(PATCH_SUB)
    scale = PENALTY * (points - 1)
    sides = 4 * slots
    cont = fc_extension.shape[0]
    inner, outer = fourier_matrix(points, cont)
    links = connectivity.T

    def stay(x):
        return pltpu.with_memory_space_constraint(jnp.asarray(x), pltpu.HBM)

    def like(x):
        return jax.ShapeDtypeStruct(x.shape, x.dtype)

    box = jax.ShapeDtypeStruct((2, 16, points), F32)
    pair = jax.ShapeDtypeStruct((2 * points, 2 * points), BF16)
    square = pltpu.VMEM((points, points), F32)
    parts = pltpu.VMEM((components, 2 * points, 2 * points), BF16)
    grid = pltpu.VMEM(fields.shape, F32)

    (b0, b1, b2, b3, own, card, rate, left, right, fields, density, moduli, diag, cross, held) = pl.pallas_call(
        functools.partial(front_kernel, total=total),
        out_shape=[box] * 4
        + [
            jax.ShapeDtypeStruct((sides, 16, points), F32),
            jax.ShapeDtypeStruct((total, points), F32),
            like(fields),
            pair,
            pair,
        ]
        + [like(x) for x in (fields, density, moduli, diag, cross, links)],
        in_specs=[ANY] * 9 + [SMEM],
        out_specs=[VMEM] * 5 + [ANY] + [VMEM] * 9,
        scratch_shapes=[
            square,
            pltpu.VMEM((points, cont), F32),
            pltpu.VMEM((points, cont), F32),
            square,
            parts,
            parts,
            grid,
            grid,
            pltpu.SMEM(links.shape, jnp.int32),
            pltpu.VMEM((total, points), F32),
            pltpu.SemaphoreType.DMA((10 + components,)),
        ],
        compiler_params=PARAMS,
        name="front",
    )(*[stay(x) for x in (fields, density, moduli, diag, cross, inner, outer, fc_extension.T, links)], patch_count)
    cards = lax.all_to_all(card, PATCH_SUB, 0, 0, tiled=True)
    arrived = [lax.ppermute(b, PATCH_SUB, route) for b, route in zip((b0, b1, b2, b3), routes(total))]
    line = pltpu.VMEM((sides, 8, points), F32)
    return pl.pallas_call(
        functools.partial(last_kernel, total=total, scale=scale),
        out_shape=like(fields),
        in_specs=[VMEM] * 14 + [SMEM] * 2,
        out_specs=ANY,
        scratch_shapes=[
            pltpu.VMEM((2 * sides, 16, points), F32),
            line,
            line,
            pltpu.VMEM((5, 2 * sides, points), F32),
            square,
            square,
            square,
            parts,
            parts,
            grid,
            grid,
            grid,
            grid,
            pltpu.SemaphoreType.DMA((components * slots,)),
        ],
        compiler_params=PARAMS,
        name="last",
    )(fields, rate, density, moduli, diag, cross, left, right, own, cards, *arrived, held, patch_count)


def solution(mesh):
    torus = Mesh(
        mesh.devices.reshape(4, 8, 4, mesh.shape["sub"]), ("patch_0", "patch_1", "patch_2", "sub")
    )
    return jax.shard_map(
        shards,
        mesh=torus,
        in_specs=(
            P(None, PATCH_SUB, None, None),
            P(PATCH_SUB, None, None),
            P(None, PATCH_SUB, None, None),
            P(None, PATCH_SUB, None, None),
            P(None, PATCH_SUB, None, None),
            P(),
            P(PATCH_SUB),
            P(PATCH_SUB, None),
        ),
        out_specs=P(None, PATCH_SUB, None, None),
        check_vma=False,
    )
```

```python
import functools

import jax
import jax.numpy as jnp
import numpy as np
from jax import lax
from jax.experimental import pallas as pl
from jax.experimental.pallas import tpu as pltpu
from jax.sharding import Mesh
from jax.sharding import PartitionSpec as P

PATCH_SUB = ("patch_0", "patch_1", "patch_2", "sub")

CFL = 0.5
PENALTY = 0.5
CHUNK = 16
F32 = jnp.float32
BF16 = jnp.bfloat16
VMEM = pl.BlockSpec(memory_space=pltpu.VMEM)
SMEM = pl.BlockSpec(memory_space=pltpu.SMEM)
ANY = pl.BlockSpec(memory_space=pltpu.HBM)
PARAMS = pltpu.CompilerParams(vmem_limit_bytes=14 * 1024 * 1024)
CONN_LANE = 40
PEAK_LANE = 64


def fourier_matrix(points, cont):
    length = points + cont
    delta = np.arange(points)[:, None] - np.arange(length)[None, :]
    safe = np.where(delta == 0, 1, delta)
    scale = np.pi * (points - 1) / length
    sign = np.where(delta % 2 == 0, 1.0, -1.0)
    full = np.where(delta == 0, 0.0, scale * sign / np.sin(np.pi * safe / length))
    return full[:, :points].astype(np.float32), full[:, points:].astype(np.float32)


def offsets(total):
    step = total // 2 + 1
    return (1, -1, step, -step)


ORDER = (3,0,1,2)


def routes(total):
    return [
        [(i, (i + (offset if i % 2 == 0 else -offset)) % total) for i in range(total)]
        for offset in (offsets(total)[k] for k in ORDER)
    ]


def partners(me, total):
    sign = jnp.where(lax.rem(me, 2) == 0, 1, -1)
    return [lax.rem(me + sign * offsets(total)[k] + total, total) for k in ORDER]


def lane_ids(shape):
    return lax.broadcasted_iota(jnp.int32, shape, len(shape) - 1)


def split(value):
    high = value.astype(BF16)
    return high, (value - high.astype(F32)).astype(BF16)


def boundary_columns(load, scr_ref, fields, slots, points):
    lanes = lane_ids((points, points))
    columns = jnp.zeros((points, points), F32)
    for s in range(slots):
        for f in range(fields):
            at = 2 * (s * fields + f)
            columns = jnp.where((lanes == at) | (lanes == at + 1), pltpu.roll(load(f, s), at + 1, 1), columns)
    scr_ref[...] = columns.T


def boundary_lines(ref, own_ref, row, scr_ref, fields, slots, points):
    boundary_columns(lambda f, s: ref[f, s], scr_ref, fields, slots, points)
    for s in range(slots):
        for f in range(fields):
            own_ref[4 * s, pl.ds(row + f, 1), :] = ref[f, s, pl.ds(0, 1), :]
            own_ref[4 * s + 1, pl.ds(row + f, 1), :] = ref[f, s, pl.ds(points - 1, 1), :]
        base = 2 * s * fields
        own_ref[4 * s + 2, pl.ds(row, fields), :] = scr_ref[pl.ds(base + 1, fields, stride=2), :]
        own_ref[4 * s + 3, pl.ds(row, fields), :] = scr_ref[pl.ds(base, fields, stride=2), :]


def column_part(turned, at, points):
    moved = pltpu.roll(turned, points - 1 - at, 1)
    lanes = lane_ids(moved.shape)
    return jnp.where((lanes == 0) | (lanes == points - 1), moved, 0.0)


def turn_jumps(jump_ref, scr_ref, fields, slots):
    for s in range(slots):
        for f in range(fields):
            at = 2 * (s * fields + f)
            scr_ref[pl.ds(at + 1, 1), :] = jump_ref[4 * s + 2, pl.ds(f, 1), :]
            scr_ref[pl.ds(at, 1), :] = jump_ref[4 * s + 3, pl.ds(f, 1), :]
    return scr_ref[...].T


def derivatives(f, value_of, left_ref, right_ref, cols_ref, rows_ref, xi_ref, eta_ref, slots, points):
    for s in range(slots):
        high, low = split(value_of(s))
        cols_ref[f, pl.ds(0, points), pl.ds(s * points, points)] = high
        cols_ref[f, pl.ds(points, points), pl.ds(s * points, points)] = low
        rows_ref[f, pl.ds(s * points, points), pl.ds(0, points)] = high
        rows_ref[f, pl.ds(s * points, points), pl.ds(points, points)] = low
    got = jnp.dot(left_ref[...], cols_ref[f], preferred_element_type=F32)
    along = got[:points] + got[points:]
    for s in range(slots):
        xi_ref[f, s] = along[:, s * points : (s + 1) * points]
    got = jnp.dot(rows_ref[f], right_ref[...], preferred_element_type=F32)
    along = got[:, :points] + got[:, points:]
    for s in range(slots):
        eta_ref[f, s] = along[s * points : (s + 1) * points]


def assemble(s, rows, density_ref, moduli_ref, diag_ref, cross_ref, xi_ref, eta_ref):
    xi_x, eta_y = diag_ref[0, s, rows, :], diag_ref[1, s, rows, :]
    xi_y, eta_x = cross_ref[0, s, rows, :], cross_ref[1, s, rows, :]
    lame, shear = moduli_ref[0, s, rows, :], moduli_ref[1, s, rows, :]
    light = 1.0 / density_ref[s, rows, :]
    stiff = lame + 2.0 * shear

    def dx(f):
        return xi_x * xi_ref[f, s, rows, :] + eta_x * eta_ref[f, s, rows, :]

    def dy(f):
        return xi_y * xi_ref[f, s, rows, :] + eta_y * eta_ref[f, s, rows, :]

    one_x, two_y = dx(0), dy(1)
    return (
        (dx(2) + dy(4)) * light,
        (dx(4) + dy(3)) * light,
        stiff * one_x + lame * two_y,
        lame * one_x + stiff * two_y,
        shear * (dy(0) + dx(1)),
    )


def build_matrices(inner, outer, ext, match, left_ref, right_ref):
    points = inner.shape[0]
    folded = lax.dot_general(
        outer, ext, (((1,), (1,)), ((), ())), precision=lax.Precision.HIGHEST, preferred_element_type=F32
    )
    full = inner + pltpu.roll(folded, points - match, 1)
    zero = jnp.zeros((points, points), BF16)
    first, second = pl.ds(0, points), pl.ds(points, points)
    high, low = split(full)
    left_ref[first, first] = high
    left_ref[first, second] = high
    left_ref[second, first] = low
    left_ref[second, second] = zero
    high, low = split(full.T)
    right_ref[first, first] = high
    right_ref[second, first] = high
    right_ref[first, second] = low
    right_ref[second, second] = zero


def front_kernel(
    fields_in, density_in, moduli_in, diag_in, cross_in, inner_in, outer_in, ext_in, conn_in, count_ref,
    out0, out1, out2, out3, own_ref, card_ref, rate_ref, left_ref, right_ref,
    fields_ref, density_ref, moduli_ref, diag_ref, cross_ref, links_ref,
    inner_ref, outer_ref, ext_ref, scr_ref, cols_ref, rows_ref, xi_ref, eta_ref, conn_ref, rows_out_ref, sems, *, total,
):
    fields, slots, points, _ = fields_ref.shape
    sides = 4 * slots

    ext_ref[...] = jnp.zeros(ext_ref.shape, F32)

    def fetch(source, target, at):
        copy = pltpu.make_async_copy(source, target, sems.at[at])
        copy.start()
        return copy

    small = [fetch(a, b, i) for i, (a, b) in enumerate(((inner_in, inner_ref), (outer_in, outer_ref), (ext_in, ext_ref.at[pl.ds(0, ext_in.shape[0])])))]
    coefs = [
        fetch(a, b, 3 + fields + i)
        for i, (a, b) in enumerate(
            ((density_in, density_ref), (moduli_in, moduli_ref), (diag_in, diag_ref), (cross_in, cross_ref))
        )
    ]
    large = [fetch(fields_in.at[f], fields_ref.at[f], 3 + f) for f in range(fields)]
    links = [fetch(conn_in, conn_ref, 7 + fields), fetch(conn_in, links_ref, 8 + fields)]
    for copy in small:
        copy.wait()
    build_matrices(inner_ref[...], outer_ref[...], ext_ref[...], ext_in.shape[0] // 2, left_ref, right_ref)
    for copy in coefs + links:
        copy.wait()

    peak = jnp.zeros((8, points), F32)
    for s in range(slots):
        live = s < count_ref[0]
        for c in range(points // CHUNK):
            rows = pl.ds(c * CHUNK, CHUNK)
            stiff = moduli_ref[0, s, rows, :] + 2.0 * moduli_ref[1, s, rows, :]
            xi_x, eta_y = diag_ref[0, s, rows, :], diag_ref[1, s, rows, :]
            xi_y, eta_x = cross_ref[0, s, rows, :], cross_ref[1, s, rows, :]
            speed = jnp.sqrt(stiff / density_ref[s, rows, :]) * (
                jnp.sqrt(xi_x * xi_x + xi_y * xi_y) + jnp.sqrt(eta_x * eta_x + eta_y * eta_y)
            )
            speed = jnp.where(live, speed, 0.0)
            for r in range(CHUNK // 8):
                peak = jnp.maximum(peak, speed[8 * r : 8 * r + 8])
    peak = jnp.max(jnp.max(peak, axis=0, keepdims=True), axis=1, keepdims=True)

    for copy in large:
        copy.wait()
    boundary_lines(fields_ref, own_ref, 0, scr_ref, fields, slots, points)
    lanes = lane_ids((8, points))
    corners = jnp.zeros((8, points), F32)
    for s in range(slots):
        for a in range(2):
            k = 4 * s + 2 * a
            moved = pltpu.roll(own_ref[4 * s + a, pl.ds(0, 8), :], k + 1, 1)
            corners = jnp.where((lanes == k) | (lanes == k + 1), moved, corners)
    scr_ref[pl.ds(0, 8), :] = corners
    lane = lane_ids((1, points))
    card = jnp.where(lane == PEAK_LANE, peak, 0.0)
    for f in range(fields):
        moved = pltpu.roll(scr_ref[pl.ds(f, 1), :], 8 * f, 1)
        card = jnp.where((lane >= 8 * f) & (lane < 8 * f + sides), moved, card)
    for i in range(sides):
        for c in range(3):
            card = jnp.where(lane == CONN_LANE + 3 * i + c, conn_ref[c, i].astype(F32), card)
    rows_out_ref[...] = jnp.broadcast_to(card, rows_out_ref.shape)
    sent = fetch(rows_out_ref, card_ref, 9 + fields)

    for f in range(fields):
        derivatives(
            f, lambda s, f=f: fields_ref[f, s], left_ref, right_ref, cols_ref, rows_ref, xi_ref, eta_ref, slots, points
        )
    for s in range(slots):
        for c in range(points // CHUNK):
            rows = pl.ds(c * CHUNK, CHUNK)
            parts = assemble(s, rows, density_ref, moduli_ref, diag_ref, cross_ref, xi_ref, eta_ref)
            for f in range(fields):
                rate_ref[f, s, rows, :] = parts[f]
    boundary_lines(rate_ref, own_ref, 8, scr_ref, fields, slots, points)

    for partner, out_ref in zip(partners(lax.axis_index(PATCH_SUB), total), (out0, out1, out2, out3)):
        first = jnp.int32(0)
        second = jnp.int32(0)
        count = jnp.int32(0)
        for i in range(sides):
            match = conn_ref[0, i] == partner
            first = jnp.where(match & (count == 0), i, first)
            second = jnp.where(match & (count == 1), i, second)
            count = count + match.astype(jnp.int32)
        out_ref[0] = own_ref[first]
        out_ref[1] = own_ref[second]
    sent.wait()


def corner_terms(cards_ref, conn_ref, near_ref, total, sides, points):
    shape = (2 * sides, points)
    rows = lax.broadcasted_iota(jnp.int32, shape, 0)
    lanes = lane_ids(shape)
    steps = (0,) + offsets(total)
    owner = jnp.zeros(shape, jnp.int32)
    strip = jnp.zeros(shape, jnp.int32)
    flip = jnp.zeros(shape, jnp.int32)
    for i in range(sides):
        here = rows // 2 == i
        held = jnp.maximum(conn_ref[0, i], 0)
        owner = jnp.where(here, held, owner)
        strip = jnp.where(here, conn_ref[1, i], strip)
        flip = jnp.where(here, conn_ref[2, i], flip)
        for d, offset in enumerate(steps):
            card = cards_ref[pl.ds(lax.rem(held + offset + total, total), 1), :]
            near_ref[d, pl.ds(2 * i, 1), :] = card
            near_ref[d, pl.ds(2 * i + 1, 1), :] = card

    def pick(array, index):
        return jnp.take_along_axis(array, index, axis=1)

    side = strip % 4
    base = strip - side
    at_end = jnp.where(rows % 2 == 0, 1 - flip, flip)
    across = side < 2
    other = jnp.where(across, 2 + at_end, at_end)
    odd = side % 2
    first = jnp.where(across, odd, at_end)
    second = jnp.where(across, at_end, odd)
    spread = 8 * jnp.minimum(lanes, 4)
    partner = near_ref[0]
    value = pick(partner, spread + base + 2 * first + 1 - second)
    link = CONN_LANE + 3 * (base + other)
    far_owner = pick(partner, link).astype(jnp.int32)
    far_strip = pick(partner, link + 1).astype(jnp.int32)
    far_flip = pick(partner, link + 2).astype(jnp.int32)
    far_card = partner
    for d, offset in enumerate(steps):
        if d:
            far_card = jnp.where(far_owner == lax.rem(owner + offset + total, total), near_ref[d], far_card)
    far_side = far_strip % 4
    far_base = far_strip - far_side
    point = jnp.where(far_flip == 1, 1 - odd, odd)
    far_across = far_side < 2
    far_odd = far_side % 2
    far_first = jnp.where(far_across, far_odd, point)
    far_second = jnp.where(far_across, point, far_odd)
    beyond = pick(far_card, spread + far_base + 2 * far_first + 1 - far_second)
    return jnp.where(far_owner >= 0, beyond - value, 0.0)


def last_kernel(
    fields_ref, inside_ref, density_ref, moduli_ref, diag_ref, cross_ref, left_ref, right_ref, own_ref, cards_ref,
    in0, in1, in2, in3, conn_ref, count_ref,
    final_out,
    table_ref, jump_ref, mine_ref, near_ref, scr_ref, turned_ref, corner_ref,
    cols_ref, rows_ref, xi_ref, eta_ref, rate_ref, final_ref, sems, *, total, scale,
):
    fields, slots, points, _ = fields_ref.shape
    sides = 4 * slots
    lanes = lane_ids((8, points))
    scr_ref[...] = jnp.zeros(scr_ref.shape, F32)

    corner_ref[...] = jnp.zeros(corner_ref.shape, F32)
    corner_ref[pl.ds(0, 2 * sides), :] = corner_terms(cards_ref, conn_ref, near_ref, total, sides, points)
    for i in range(sides):
        table_ref[i] = own_ref[i]
    for k, in_ref in enumerate((in0, in1, in2, in3)):
        table_ref[sides + 2 * k] = in_ref[0]
        table_ref[sides + 2 * k + 1] = in_ref[1]
    weights = []
    partner_rates = []
    for i in range(sides):
        owner = conn_ref[0, i]
        strip = conn_ref[1, i]
        position = jnp.int32(0)
        for j in range(sides):
            if j != i:
                before = (conn_ref[0, j] == owner) & (conn_ref[1, j] < strip)
                position = position + before.astype(jnp.int32)
        place = strip
        for k, partner in enumerate(partners(lax.axis_index(PATCH_SUB), total)):
            place = jnp.where(owner == partner, sides + 2 * k + position, place)
        place = jnp.clip(place, 0, 2 * sides - 1)
        index = jnp.where(conn_ref[2, i] == 1, points - 1 - lanes, lanes)
        line = jnp.take_along_axis(table_ref[place, pl.ds(0, 8), :], index, axis=1)
        rate = jnp.take_along_axis(table_ref[place, pl.ds(8, 8), :], index, axis=1)
        weight = jnp.where(owner >= 0, scale, 0.0).astype(F32)
        jump = weight * (line - own_ref[i, pl.ds(0, 8), :])
        jump_ref[i] = jump
        weights.append(weight)
        partner_rates.append(rate - jump)
    turned_ref[...] = turn_jumps(jump_ref, scr_ref, fields, slots)

    for f in range(fields):
        for s in range(slots):
            rate_ref[f, s] = inside_ref[f, s] + column_part(turned_ref[...], 2 * (s * fields + f), points)
            for side, row in ((0, 0), (1, points - 1)):
                line = rate_ref[f, s, pl.ds(row, 1), :] + jump_ref[4 * s + side, pl.ds(f, 1), :]
                rate_ref[f, s, pl.ds(row, 1), :] = line
        derivatives(
            f, lambda s, f=f: rate_ref[f, s], left_ref, right_ref, cols_ref, rows_ref, xi_ref, eta_ref, slots, points
        )
    boundary_lines(rate_ref, mine_ref, 0, scr_ref, fields, slots, points)

    bound = jnp.max(cards_ref[...], axis=0, keepdims=True)
    bound = jnp.where(lane_ids(bound.shape) == PEAK_LANE, bound, 0.0)
    bound = jnp.max(bound, axis=1, keepdims=True)
    dt = CFL / (bound * (points - 1))
    half = 0.5 * dt * dt

    corners = corner_ref[...].T[:8]
    for i in range(sides):
        partner = partner_rates[i] + scale * column_part(corners, 2 * i, points)
        jump_ref[i] = half * weights[i] * (partner - mine_ref[i])
    turned_ref[...] = turn_jumps(jump_ref, scr_ref, fields, slots)

    copies = []
    for s in range(slots):
        live = s < count_ref[0]
        for c in range(points // CHUNK):
            rows = pl.ds(c * CHUNK, CHUNK)
            parts = assemble(s, rows, density_ref, moduli_ref, diag_ref, cross_ref, xi_ref, eta_ref)
            for f in range(fields):
                value = fields_ref[f, s, rows, :] + dt * rate_ref[f, s, rows, :] + half * parts[f]
                value = value + column_part(turned_ref[rows, :], 2 * (s * fields + f), points)
                final_ref[f, s, rows, :] = jnp.where(live, value, 0.0)
        for f in range(fields):
            for side, row in ((0, 0), (1, points - 1)):
                line = final_ref[f, s, pl.ds(row, 1), :] + jump_ref[4 * s + side, pl.ds(f, 1), :]
                final_ref[f, s, pl.ds(row, 1), :] = jnp.where(live, line, 0.0)
            copy = pltpu.make_async_copy(final_ref.at[f, s], final_out.at[f, s], sems.at[s * fields + f])
            copy.start()
            copies.append(copy)
    for copy in copies:
        copy.wait()


def shards(fields, density, moduli, diag, cross, fc_extension, patch_count, connectivity):
    components, slots, points, _ = fields.shape
    total = lax.axis_size(PATCH_SUB)
    scale = PENALTY * (points - 1)
    sides = 4 * slots
    cont = fc_extension.shape[0]
    inner, outer = fourier_matrix(points, cont)
    links = connectivity.T

    def stay(x):
        return pltpu.with_memory_space_constraint(jnp.asarray(x), pltpu.HBM)

    def like(x):
        return jax.ShapeDtypeStruct(x.shape, x.dtype)

    box = jax.ShapeDtypeStruct((2, 16, points), F32)
    pair = jax.ShapeDtypeStruct((2 * points, 2 * points), BF16)
    square = pltpu.VMEM((points, points), F32)
    parts = pltpu.VMEM((components, 2 * points, 2 * points), BF16)
    grid = pltpu.VMEM(fields.shape, F32)

    (b0, b1, b2, b3, own, card, rate, left, right, fields, density, moduli, diag, cross, held) = pl.pallas_call(
        functools.partial(front_kernel, total=total),
        out_shape=[box] * 4
        + [
            jax.ShapeDtypeStruct((sides, 16, points), F32),
            jax.ShapeDtypeStruct((total, points), F32),
            like(fields),
            pair,
            pair,
        ]
        + [like(x) for x in (fields, density, moduli, diag, cross, links)],
        in_specs=[ANY] * 9 + [SMEM],
        out_specs=[VMEM] * 5 + [ANY] + [VMEM] * 9,
        scratch_shapes=[
            square,
            pltpu.VMEM((points, cont), F32),
            pltpu.VMEM((points, cont), F32),
            square,
            parts,
            parts,
            grid,
            grid,
            pltpu.SMEM(links.shape, jnp.int32),
            pltpu.VMEM((total, points), F32),
            pltpu.SemaphoreType.DMA((10 + components,)),
        ],
        compiler_params=PARAMS,
        name="front",
    )(*[stay(x) for x in (fields, density, moduli, diag, cross, inner, outer, fc_extension.T, links)], patch_count)
    cards = lax.all_to_all(card, PATCH_SUB, 0, 0, tiled=True)
    arrived = [lax.ppermute(b, PATCH_SUB, route) for b, route in zip((b0, b1, b2, b3), routes(total))]
    line = pltpu.VMEM((sides, 8, points), F32)
    return pl.pallas_call(
        functools.partial(last_kernel, total=total, scale=scale),
        out_shape=like(fields),
        in_specs=[VMEM] * 14 + [SMEM] * 2,
        out_specs=ANY,
        scratch_shapes=[
            pltpu.VMEM((2 * sides, 16, points), F32),
            line,
            line,
            pltpu.VMEM((5, 2 * sides, points), F32),
            square,
            square,
            square,
            parts,
            parts,
            grid,
            grid,
            grid,
            grid,
            pltpu.SemaphoreType.DMA((components * slots,)),
        ],
        compiler_params=PARAMS,
        name="last",
    )(fields, rate, density, moduli, diag, cross, left, right, own, cards, *arrived, held, patch_count)


def solution(mesh):
    torus = Mesh(
        mesh.devices.reshape(4, 8, 4, mesh.shape["sub"]), ("patch_0", "patch_1", "patch_2", "sub")
    )
    return jax.shard_map(
        shards,
        mesh=torus,
        in_specs=(
            P(None, PATCH_SUB, None, None),
            P(PATCH_SUB, None, None),
            P(None, PATCH_SUB, None, None),
            P(None, PATCH_SUB, None, None),
            P(None, PATCH_SUB, None, None),
            P(),
            P(PATCH_SUB),
            P(PATCH_SUB, None),
        ),
        out_specs=P(None, PATCH_SUB, None, None),
        check_vma=False,
    )
```

```python
import functools

import jax
import jax.numpy as jnp
import numpy as np
from jax import lax
from jax.experimental import pallas as pl
from jax.experimental.pallas import tpu as pltpu
from jax.sharding import Mesh
from jax.sharding import PartitionSpec as P

PATCH_SUB = ("patch_0", "patch_1", "patch_2", "sub")

CFL = 0.5
PENALTY = 0.5
CHUNK = 32
F32 = jnp.float32
BF16 = jnp.bfloat16
VMEM = pl.BlockSpec(memory_space=pltpu.VMEM)
SMEM = pl.BlockSpec(memory_space=pltpu.SMEM)
ANY = pl.BlockSpec(memory_space=pltpu.HBM)
PARAMS = pltpu.CompilerParams(vmem_limit_bytes=14 * 1024 * 1024)
CONN_LANE = 40
PEAK_LANE = 64


def fourier_matrix(points, cont):
    length = points + cont
    delta = np.arange(points)[:, None] - np.arange(length)[None, :]
    safe = np.where(delta == 0, 1, delta)
    scale = np.pi * (points - 1) / length
    sign = np.where(delta % 2 == 0, 1.0, -1.0)
    full = np.where(delta == 0, 0.0, scale * sign / np.sin(np.pi * safe / length))
    return full[:, :points].astype(np.float32), full[:, points:].astype(np.float32)


def offsets(total):
    step = total // 2 + 1
    return (1, -1, step, -step)


ORDER = (3, 1, 2, 0)


def routes(total):
    return [
        [(i, (i + (offset if i % 2 == 0 else -offset)) % total) for i in range(total)]
        for offset in (offsets(total)[k] for k in ORDER)
    ]


def partners(me, total):
    sign = jnp.where(lax.rem(me, 2) == 0, 1, -1)
    return [lax.rem(me + sign * offsets(total)[k] + total, total) for k in ORDER]


def lane_ids(shape):
    return lax.broadcasted_iota(jnp.int32, shape, len(shape) - 1)


def split(value):
    high = value.astype(BF16)
    return high, (value - high.astype(F32)).astype(BF16)


def boundary_columns(load, scr_ref, fields, slots, points):
    lanes = lane_ids((points, points))
    columns = jnp.zeros((points, points), F32)
    for s in range(slots):
        for f in range(fields):
            at = 2 * (s * fields + f)
            columns = jnp.where((lanes == at) | (lanes == at + 1), pltpu.roll(load(f, s), at + 1, 1), columns)
    scr_ref[...] = columns.T


def boundary_lines(ref, own_ref, row, scr_ref, fields, slots, points):
    boundary_columns(lambda f, s: ref[f, s], scr_ref, fields, slots, points)
    for s in range(slots):
        for f in range(fields):
            own_ref[4 * s, pl.ds(row + f, 1), :] = ref[f, s, pl.ds(0, 1), :]
            own_ref[4 * s + 1, pl.ds(row + f, 1), :] = ref[f, s, pl.ds(points - 1, 1), :]
        base = 2 * s * fields
        own_ref[4 * s + 2, pl.ds(row, fields), :] = scr_ref[pl.ds(base + 1, fields, stride=2), :]
        own_ref[4 * s + 3, pl.ds(row, fields), :] = scr_ref[pl.ds(base, fields, stride=2), :]


def column_part(turned, at, points):
    moved = pltpu.roll(turned, points - 1 - at, 1)
    lanes = lane_ids(moved.shape)
    return jnp.where((lanes == 0) | (lanes == points - 1), moved, 0.0)


def turn_jumps(jump_ref, scr_ref, fields, slots):
    for s in range(slots):
        for f in range(fields):
            at = 2 * (s * fields + f)
            scr_ref[pl.ds(at + 1, 1), :] = jump_ref[4 * s + 2, pl.ds(f, 1), :]
            scr_ref[pl.ds(at, 1), :] = jump_ref[4 * s + 3, pl.ds(f, 1), :]
    return scr_ref[...].T


def derivatives(f, value_of, left_ref, right_ref, cols_ref, rows_ref, xi_ref, eta_ref, slots, points):
    for s in range(slots):
        high, low = split(value_of(s))
        cols_ref[f, pl.ds(0, points), pl.ds(s * points, points)] = high
        cols_ref[f, pl.ds(points, points), pl.ds(s * points, points)] = low
        rows_ref[f, pl.ds(s * points, points), pl.ds(0, points)] = high
        rows_ref[f, pl.ds(s * points, points), pl.ds(points, points)] = low
    got = jnp.dot(left_ref[...], cols_ref[f], preferred_element_type=F32)
    along = got[:points] + got[points:]
    for s in range(slots):
        xi_ref[f, s] = along[:, s * points : (s + 1) * points]
    got = jnp.dot(rows_ref[f], right_ref[...], preferred_element_type=F32)
    along = got[:, :points] + got[:, points:]
    for s in range(slots):
        eta_ref[f, s] = along[s * points : (s + 1) * points]


def assemble(s, rows, density_ref, moduli_ref, diag_ref, cross_ref, xi_ref, eta_ref):
    xi_x, eta_y = diag_ref[0, s, rows, :], diag_ref[1, s, rows, :]
    xi_y, eta_x = cross_ref[0, s, rows, :], cross_ref[1, s, rows, :]
    lame, shear = moduli_ref[0, s, rows, :], moduli_ref[1, s, rows, :]
    light = 1.0 / density_ref[s, rows, :]
    stiff = lame + 2.0 * shear

    def dx(f):
        return xi_x * xi_ref[f, s, rows, :] + eta_x * eta_ref[f, s, rows, :]

    def dy(f):
        return xi_y * xi_ref[f, s, rows, :] + eta_y * eta_ref[f, s, rows, :]

    one_x, two_y = dx(0), dy(1)
    return (
        (dx(2) + dy(4)) * light,
        (dx(4) + dy(3)) * light,
        stiff * one_x + lame * two_y,
        lame * one_x + stiff * two_y,
        shear * (dy(0) + dx(1)),
    )


def build_matrices(inner, outer, ext, match, left_ref, right_ref):
    points = inner.shape[0]
    folded = lax.dot_general(
        outer, ext, (((1,), (1,)), ((), ())), precision=lax.Precision.HIGHEST, preferred_element_type=F32
    )
    full = inner + pltpu.roll(folded, points - match, 1)
    zero = jnp.zeros((points, points), BF16)
    first, second = pl.ds(0, points), pl.ds(points, points)
    high, low = split(full)
    left_ref[first, first] = high
    left_ref[first, second] = high
    left_ref[second, first] = low
    left_ref[second, second] = zero
    high, low = split(full.T)
    right_ref[first, first] = high
    right_ref[second, first] = high
    right_ref[first, second] = low
    right_ref[second, second] = zero


def front_kernel(
    fields_in, density_in, moduli_in, diag_in, cross_in, inner_in, outer_in, ext_in, conn_in, count_ref,
    out0, out1, out2, out3, own_ref, card_ref, rate_ref, left_ref, right_ref,
    fields_ref, density_ref, moduli_ref, diag_ref, cross_ref, links_ref,
    inner_ref, outer_ref, ext_ref, scr_ref, cols_ref, rows_ref, xi_ref, eta_ref, conn_ref, rows_out_ref, sems, *, total,
):
    fields, slots, points, _ = fields_ref.shape
    sides = 4 * slots

    ext_ref[...] = jnp.zeros(ext_ref.shape, F32)

    def fetch(source, target, at):
        copy = pltpu.make_async_copy(source, target, sems.at[at])
        copy.start()
        return copy

    small = [fetch(a, b, i) for i, (a, b) in enumerate(((inner_in, inner_ref), (outer_in, outer_ref), (ext_in, ext_ref.at[pl.ds(0, ext_in.shape[0])])))]
    coefs = [
        fetch(a, b, 3 + fields + i)
        for i, (a, b) in enumerate(
            ((density_in, density_ref), (moduli_in, moduli_ref), (diag_in, diag_ref), (cross_in, cross_ref))
        )
    ]
    large = [fetch(fields_in.at[f], fields_ref.at[f], 3 + f) for f in range(fields)]
    links = [fetch(conn_in, conn_ref, 7 + fields), fetch(conn_in, links_ref, 8 + fields)]
    for copy in small:
        copy.wait()
    build_matrices(inner_ref[...], outer_ref[...], ext_ref[...], ext_in.shape[0] // 2, left_ref, right_ref)
    for copy in coefs + links:
        copy.wait()

    peak = jnp.zeros((8, points), F32)
    for s in range(slots):
        live = s < count_ref[0]
        for c in range(points // CHUNK):
            rows = pl.ds(c * CHUNK, CHUNK)
            stiff = moduli_ref[0, s, rows, :] + 2.0 * moduli_ref[1, s, rows, :]
            xi_x, eta_y = diag_ref[0, s, rows, :], diag_ref[1, s, rows, :]
            xi_y, eta_x = cross_ref[0, s, rows, :], cross_ref[1, s, rows, :]
            speed = jnp.sqrt(stiff / density_ref[s, rows, :]) * (
                jnp.sqrt(xi_x * xi_x + xi_y * xi_y) + jnp.sqrt(eta_x * eta_x + eta_y * eta_y)
            )
            speed = jnp.where(live, speed, 0.0)
            for r in range(CHUNK // 8):
                peak = jnp.maximum(peak, speed[8 * r : 8 * r + 8])
    peak = jnp.max(jnp.max(peak, axis=0, keepdims=True), axis=1, keepdims=True)

    for copy in large:
        copy.wait()
    boundary_lines(fields_ref, own_ref, 0, scr_ref, fields, slots, points)
    lanes = lane_ids((8, points))
    corners = jnp.zeros((8, points), F32)
    for s in range(slots):
        for a in range(2):
            k = 4 * s + 2 * a
            moved = pltpu.roll(own_ref[4 * s + a, pl.ds(0, 8), :], k + 1, 1)
            corners = jnp.where((lanes == k) | (lanes == k + 1), moved, corners)
    scr_ref[pl.ds(0, 8), :] = corners
    lane = lane_ids((1, points))
    card = jnp.where(lane == PEAK_LANE, peak, 0.0)
    for f in range(fields):
        moved = pltpu.roll(scr_ref[pl.ds(f, 1), :], 8 * f, 1)
        card = jnp.where((lane >= 8 * f) & (lane < 8 * f + sides), moved, card)
    for i in range(sides):
        for c in range(3):
            card = jnp.where(lane == CONN_LANE + 3 * i + c, conn_ref[c, i].astype(F32), card)
    rows_out_ref[...] = jnp.broadcast_to(card, rows_out_ref.shape)
    sent = fetch(rows_out_ref, card_ref, 9 + fields)

    for f in range(fields):
        derivatives(
            f, lambda s, f=f: fields_ref[f, s], left_ref, right_ref, cols_ref, rows_ref, xi_ref, eta_ref, slots, points
        )
    for s in range(slots):
        for c in range(points // CHUNK):
            rows = pl.ds(c * CHUNK, CHUNK)
            parts = assemble(s, rows, density_ref, moduli_ref, diag_ref, cross_ref, xi_ref, eta_ref)
            for f in range(fields):
                rate_ref[f, s, rows, :] = parts[f]
    boundary_lines(rate_ref, own_ref, 8, scr_ref, fields, slots, points)

    for partner, out_ref in zip(partners(lax.axis_index(PATCH_SUB), total), (out0, out1, out2, out3)):
        first = jnp.int32(0)
        second = jnp.int32(0)
        count = jnp.int32(0)
        for i in range(sides):
            match = conn_ref[0, i] == partner
            first = jnp.where(match & (count == 0), i, first)
            second = jnp.where(match & (count == 1), i, second)
            count = count + match.astype(jnp.int32)
        out_ref[0] = own_ref[first]
        out_ref[1] = own_ref[second]
    sent.wait()


def corner_terms(cards_ref, conn_ref, near_ref, total, sides, points):
    shape = (2 * sides, points)
    rows = lax.broadcasted_iota(jnp.int32, shape, 0)
    lanes = lane_ids(shape)
    steps = (0,) + offsets(total)
    owner = jnp.zeros(shape, jnp.int32)
    strip = jnp.zeros(shape, jnp.int32)
    flip = jnp.zeros(shape, jnp.int32)
    for i in range(sides):
        here = rows // 2 == i
        held = jnp.maximum(conn_ref[0, i], 0)
        owner = jnp.where(here, held, owner)
        strip = jnp.where(here, conn_ref[1, i], strip)
        flip = jnp.where(here, conn_ref[2, i], flip)
        for d, offset in enumerate(steps):
            card = cards_ref[pl.ds(lax.rem(held + offset + total, total), 1), :]
            near_ref[d, pl.ds(2 * i, 1), :] = card
            near_ref[d, pl.ds(2 * i + 1, 1), :] = card

    def pick(array, index):
        return jnp.take_along_axis(array, index, axis=1)

    side = strip % 4
    base = strip - side
    at_end = jnp.where(rows % 2 == 0, 1 - flip, flip)
    across = side < 2
    other = jnp.where(across, 2 + at_end, at_end)
    odd = side % 2
    first = jnp.where(across, odd, at_end)
    second = jnp.where(across, at_end, odd)
    spread = 8 * jnp.minimum(lanes, 4)
    partner = near_ref[0]
    value = pick(partner, spread + base + 2 * first + 1 - second)
    link = CONN_LANE + 3 * (base + other)
    far_owner = pick(partner, link).astype(jnp.int32)
    far_strip = pick(partner, link + 1).astype(jnp.int32)
    far_flip = pick(partner, link + 2).astype(jnp.int32)
    far_card = partner
    for d, offset in enumerate(steps):
        if d:
            far_card = jnp.where(far_owner == lax.rem(owner + offset + total, total), near_ref[d], far_card)
    far_side = far_strip % 4
    far_base = far_strip - far_side
    point = jnp.where(far_flip == 1, 1 - odd, odd)
    far_across = far_side < 2
    far_odd = far_side % 2
    far_first = jnp.where(far_across, far_odd, point)
    far_second = jnp.where(far_across, point, far_odd)
    beyond = pick(far_card, spread + far_base + 2 * far_first + 1 - far_second)
    return jnp.where(far_owner >= 0, beyond - value, 0.0)


def last_kernel(
    fields_ref, inside_ref, density_ref, moduli_ref, diag_ref, cross_ref, left_ref, right_ref, own_ref, cards_ref,
    in0, in1, in2, in3, conn_ref, count_ref,
    final_out,
    table_ref, jump_ref, mine_ref, near_ref, scr_ref, turned_ref, corner_ref,
    cols_ref, rows_ref, xi_ref, eta_ref, rate_ref, final_ref, sems, *, total, scale,
):
    fields, slots, points, _ = fields_ref.shape
    sides = 4 * slots
    lanes = lane_ids((8, points))
    scr_ref[...] = jnp.zeros(scr_ref.shape, F32)

    for i in range(sides):
        table_ref[i] = own_ref[i]
    for k, in_ref in enumerate((in0, in1, in2, in3)):
        table_ref[sides + 2 * k] = in_ref[0]
        table_ref[sides + 2 * k + 1] = in_ref[1]
    weights = []
    partner_rates = []
    for i in range(sides):
        owner = conn_ref[0, i]
        strip = conn_ref[1, i]
        position = jnp.int32(0)
        for j in range(sides):
            if j != i:
                before = (conn_ref[0, j] == owner) & (conn_ref[1, j] < strip)
                position = position + before.astype(jnp.int32)
        place = strip
        for k, partner in enumerate(partners(lax.axis_index(PATCH_SUB), total)):
            place = jnp.where(owner == partner, sides + 2 * k + position, place)
        place = jnp.clip(place, 0, 2 * sides - 1)
        index = jnp.where(conn_ref[2, i] == 1, points - 1 - lanes, lanes)
        line = jnp.take_along_axis(table_ref[place, pl.ds(0, 8), :], index, axis=1)
        rate = jnp.take_along_axis(table_ref[place, pl.ds(8, 8), :], index, axis=1)
        weight = jnp.where(owner >= 0, scale, 0.0).astype(F32)
        jump = weight * (line - own_ref[i, pl.ds(0, 8), :])
        jump_ref[i] = jump
        weights.append(weight)
        partner_rates.append(rate - jump)
    turned_ref[...] = turn_jumps(jump_ref, scr_ref, fields, slots)

    for f in range(fields):
        for s in range(slots):
            rate_ref[f, s] = inside_ref[f, s] + column_part(turned_ref[...], 2 * (s * fields + f), points)
            for side, row in ((0, 0), (1, points - 1)):
                line = rate_ref[f, s, pl.ds(row, 1), :] + jump_ref[4 * s + side, pl.ds(f, 1), :]
                rate_ref[f, s, pl.ds(row, 1), :] = line
        derivatives(
            f, lambda s, f=f: rate_ref[f, s], left_ref, right_ref, cols_ref, rows_ref, xi_ref, eta_ref, slots, points
        )
    boundary_lines(rate_ref, mine_ref, 0, scr_ref, fields, slots, points)

    bound = jnp.max(cards_ref[...], axis=0, keepdims=True)
    bound = jnp.where(lane_ids(bound.shape) == PEAK_LANE, bound, 0.0)
    bound = jnp.max(bound, axis=1, keepdims=True)
    dt = CFL / (bound * (points - 1))
    half = 0.5 * dt * dt

    corner_ref[...] = jnp.zeros(corner_ref.shape, F32)
    corner_ref[pl.ds(0, 2 * sides), :] = corner_terms(cards_ref, conn_ref, near_ref, total, sides, points)
    corners = corner_ref[...].T[:8]
    for i in range(sides):
        partner = partner_rates[i] + scale * column_part(corners, 2 * i, points)
        jump_ref[i] = half * weights[i] * (partner - mine_ref[i])
    turned_ref[...] = turn_jumps(jump_ref, scr_ref, fields, slots)

    copies = []
    for s in range(slots):
        live = s < count_ref[0]
        for c in range(points // CHUNK):
            rows = pl.ds(c * CHUNK, CHUNK)
            parts = assemble(s, rows, density_ref, moduli_ref, diag_ref, cross_ref, xi_ref, eta_ref)
            for f in range(fields):
                value = fields_ref[f, s, rows, :] + dt * rate_ref[f, s, rows, :] + half * parts[f]
                value = value + column_part(turned_ref[rows, :], 2 * (s * fields + f), points)
                final_ref[f, s, rows, :] = jnp.where(live, value, 0.0)
        for f in range(fields):
            for side, row in ((0, 0), (1, points - 1)):
                line = final_ref[f, s, pl.ds(row, 1), :] + jump_ref[4 * s + side, pl.ds(f, 1), :]
                final_ref[f, s, pl.ds(row, 1), :] = jnp.where(live, line, 0.0)
            copy = pltpu.make_async_copy(final_ref.at[f, s], final_out.at[f, s], sems.at[s * fields + f])
            copy.start()
            copies.append(copy)
    for copy in copies:
        copy.wait()


def shards(fields, density, moduli, diag, cross, fc_extension, patch_count, connectivity):
    components, slots, points, _ = fields.shape
    total = lax.axis_size(PATCH_SUB)
    scale = PENALTY * (points - 1)
    sides = 4 * slots
    cont = fc_extension.shape[0]
    inner, outer = fourier_matrix(points, cont)
    links = connectivity.T

    def stay(x):
        return pltpu.with_memory_space_constraint(jnp.asarray(x), pltpu.HBM)

    def like(x):
        return jax.ShapeDtypeStruct(x.shape, x.dtype)

    box = jax.ShapeDtypeStruct((2, 16, points), F32)
    pair = jax.ShapeDtypeStruct((2 * points, 2 * points), BF16)
    square = pltpu.VMEM((points, points), F32)
    parts = pltpu.VMEM((components, 2 * points, 2 * points), BF16)
    grid = pltpu.VMEM(fields.shape, F32)

    (b0, b1, b2, b3, own, card, rate, left, right, fields, density, moduli, diag, cross, held) = pl.pallas_call(
        functools.partial(front_kernel, total=total),
        out_shape=[box] * 4
        + [
            jax.ShapeDtypeStruct((sides, 16, points), F32),
            jax.ShapeDtypeStruct((total, points), F32),
            like(fields),
            pair,
            pair,
        ]
        + [like(x) for x in (fields, density, moduli, diag, cross, links)],
        in_specs=[ANY] * 9 + [SMEM],
        out_specs=[VMEM] * 5 + [ANY] + [VMEM] * 9,
        scratch_shapes=[
            square,
            pltpu.VMEM((points, cont), F32),
            pltpu.VMEM((points, cont), F32),
            square,
            parts,
            parts,
            grid,
            grid,
            pltpu.SMEM(links.shape, jnp.int32),
            pltpu.VMEM((total, points), F32),
            pltpu.SemaphoreType.DMA((10 + components,)),
        ],
        compiler_params=PARAMS,
        name="front",
    )(*[stay(x) for x in (fields, density, moduli, diag, cross, inner, outer, fc_extension.T, links)], patch_count)
    cards = lax.all_to_all(card, PATCH_SUB, 0, 0, tiled=True)
    arrived = [lax.ppermute(b, PATCH_SUB, route) for b, route in zip((b0, b1, b2, b3), routes(total))]
    line = pltpu.VMEM((sides, 8, points), F32)
    return pl.pallas_call(
        functools.partial(last_kernel, total=total, scale=scale),
        out_shape=like(fields),
        in_specs=[VMEM] * 14 + [SMEM] * 2,
        out_specs=ANY,
        scratch_shapes=[
            pltpu.VMEM((2 * sides, 16, points), F32),
            line,
            line,
            pltpu.VMEM((5, 2 * sides, points), F32),
            square,
            square,
            square,
            parts,
            parts,
            grid,
            grid,
            grid,
            grid,
            pltpu.SemaphoreType.DMA((components * slots,)),
        ],
        compiler_params=PARAMS,
        name="last",
    )(fields, rate, density, moduli, diag, cross, left, right, own, cards, *arrived, held, patch_count)


def solution(mesh):
    torus = Mesh(
        mesh.devices.reshape(4, 8, 4, mesh.shape["sub"]), ("patch_0", "patch_1", "patch_2", "sub")
    )
    return jax.shard_map(
        shards,
        mesh=torus,
        in_specs=(
            P(None, PATCH_SUB, None, None),
            P(PATCH_SUB, None, None),
            P(None, PATCH_SUB, None, None),
            P(None, PATCH_SUB, None, None),
            P(None, PATCH_SUB, None, None),
            P(),
            P(PATCH_SUB),
            P(PATCH_SUB, None),
        ),
        out_specs=P(None, PATCH_SUB, None, None),
        check_vma=False,
    )
```
